32 devices in a mesh: rep: 2 (over y), ada: 4 (over z), tp: 4 (over x, core).
Axes of the slice: x: 2, y: 2, z: 4, core: 2. Of those that a mesh axis runs over, the one named last changes fastest.
Arguments:
- hidden: bfloat16 [256, 8192], P(('rep', 'ada')), parts along dimension 0, may hold values from -6 to 6
- input_norm_gain: bfloat16 [8192], replicated, may hold values from 0.5 to 1.5
- request_adapter: int32 [256], P(('rep', 'ada')), parts along dimension 0, may hold values from 0 to 15, as said below
- cache_fill_length: int32 [256], P(('rep', 'ada')), parts along dimension 0, may hold values from 1 to 512, as said below
- query_weight: bfloat16 [8192, 8192], P('ada', 'tp'), may hold values from -0.0625 to 0.0625
- key_weight: bfloat16 [8192, 1024], P('ada', 'tp'), may hold values from -0.0625 to 0.0625
- value_weight: bfloat16 [8192, 1024], P('ada', 'tp'), may hold values from -0.0625 to 0.0625
- output_weight: bfloat16 [8192, 8192], P('tp', 'ada'), may hold values from -0.0625 to 0.0625
- down_weight_all: bfloat16 [8192, 512], P('tp', 'ada'), may hold values from -0.0625 to 0.0625
- query_up_weight: bfloat16 [256, 8192], P('ada', 'tp'), may hold values from -1.5 to 1.5
- value_up_weight: bfloat16 [256, 1024], P('ada', 'tp'), may hold values from -1.5 to 1.5
- rotated_key_cache: bfloat16 [256, 512, 1024], P(('rep', 'ada'), None, 'tp'), parts along dimension 0, may hold values from -768 to 768
- stored_value_cache: bfloat16 [256, 512, 1024], P(('rep', 'ada'), None, 'tp'), parts along dimension 0, may hold values from -6 to 6
Outputs:
- layer_out: bfloat16 [256, 8192], P(('rep', 'tp'), 'ada'), parts along dimension 0
- new_key: bfloat16 [256, 1024], P(('rep', 'ada'), 'tp'), parts along dimension 0
- new_value: bfloat16 [256, 1024], P(('rep', 'ada'), 'tp'), parts along dimension 0
The draws below stay inside these ranges and needn't reach their ends.
There are 2 independent parts, one for each index of `rep`. The reference program is written for one: setup_inputs(seed, part) draws one part's arguments, and reference() takes and returns one part's arrays. A program takes and returns all parts, laid end to end along the dimension named above; an argument that names none is the same for every part. Nothing has to cross between parts.
Inputs may be any that keep to these rules, and one draw needn't show every extreme that they name: `request_adapter`: among the 32 requests of one ada index (aligned blocks), at most 16 name adapters of one group 4 * o to 4 * o + 3; in every draw one group is named by exactly 16 requests of every block. `cache_fill_length`: within each part of rep the 128 lengths sum to 32768, and some request of each part has exactly 512.
All inputs are finite; a program needn't handle non-finite values.
Results may differ from the reference program's by a relative error of at most 0.012.
The reference program's roundings to bfloat16 on the way count: a program that leaves them out, or rounds other values in their place, can miss the bound.
Values may be sent and summed in bfloat16 or wider, within the bound.
A program may use at most 64 MiB of HBM per device.

```python
import jax
import jax.numpy as jnp
from jax import lax

MODEL_WIDTH = 8192
QUERY_HEAD_COUNT = 64
KEY_VALUE_HEADS = 8
HEAD_WIDTH = 128
ADAPTER_RANK = 16
ADP_DEV = 4
REQ_DEV = 32
CTX = 512
ADAPTER_COUNT = 16
REQUESTS = 128
CAP = 16


def block_owners(block_key, owner_rank, blocks_count):
    pool_owner = jnp.repeat(jnp.arange(blocks_count, dtype=jnp.int32), CAP)
    pool_size = blocks_count * CAP
    noise_term = jax.random.randint(jax.random.fold_in(block_key, 1), (pool_size,), 0, 4096)
    rank_of = owner_rank[pool_owner]
    score_value = noise_term + jnp.where(rank_of < 4, 4096, 0) + jnp.where(rank_of == 0, 8192, 0)
    distinct = score_value * pool_size + jnp.arange(pool_size, dtype=jnp.int32)
    ranking = jnp.argsort(-distinct)
    picked = pool_owner[ranking[:REQ_DEV]]
    shuffle = jax.random.permutation(jax.random.fold_in(block_key, 2), REQ_DEV)
    return picked[shuffle]


def draw_request_adapter(key, part):
    blocks_count = REQUESTS // REQ_DEV
    order_owners = jax.random.permutation(jax.random.fold_in(key, 11), blocks_count)
    owner_rank = jnp.argsort(order_owners).astype(jnp.int32)
    block_keys = jax.random.split(jax.random.fold_in(key, 12), blocks_count)
    owners = jax.vmap(lambda block_key: block_owners(block_key, owner_rank, blocks_count))(block_keys)
    sub_index = jax.random.randint(jax.random.fold_in(key, 13), (blocks_count, REQ_DEV), 0, ADP_DEV)
    return (owners * ADP_DEV + sub_index).reshape(REQUESTS).astype(jnp.int32)


def draw_cache_fill_length(key, part):
    others = REQUESTS - 1
    remaining = REQUESTS * CTX // 2 - CTX
    base_len = remaining // others
    extra_count = remaining - others * base_len
    lengths_rest = base_len + (jnp.arange(others, dtype=jnp.int32) < extra_count).astype(jnp.int32)
    reach = min(base_len - 1, CTX - base_len - 2)
    half_count = others // 2
    shifts = jax.random.randint(jax.random.fold_in(key, 31), (half_count,), -reach, reach + 1).astype(jnp.int32)
    lengths_rest = lengths_rest.at[:half_count].add(shifts)
    lengths_rest = lengths_rest.at[half_count:2 * half_count].add(-shifts)
    lengths_rest = lengths_rest[jax.random.permutation(jax.random.fold_in(key, 32), others)]
    complete = jnp.concatenate([jnp.full((1,), CTX, jnp.int32), lengths_rest.astype(jnp.int32)])
    return complete[jax.random.permutation(jax.random.fold_in(key, 33), REQUESTS)].astype(jnp.int32)


def draw_rotated_key_cache(key, part):
    drawn = jax.random.normal(jax.random.fold_in(key, 21), (REQUESTS, CTX, KEY_VALUE_HEADS * HEAD_WIDTH), jnp.float32)
    drawn = jnp.clip(drawn, -6.0, 6.0)
    return drawn.astype(jnp.bfloat16)


def block_scale(own_key, dims, shards, least, largest):
    def one(dim, blocks):
        steps = jax.random.uniform(jax.random.fold_in(jax.random.fold_in(own_key, 6), dim), (blocks,), jnp.float32, least / len(shards), largest / len(shards))
        return jnp.repeat(jnp.exp(steps), dims[dim] // blocks).reshape((-1,) + (1,) * (len(dims) - dim - 1))

    factor_of = one(*shards[0])
    for cut in shards[1:]:
        factor_of = factor_of * one(*cut)
    return factor_of


def gaussian(own_key, extent, spread, bound, cuts=(), kind=jnp.bfloat16):
    result = jax.random.normal(own_key, extent, jnp.float32) * spread
    if len(cuts) > 0:
        result = block_scale(own_key, extent, cuts, -0.22, 0.18) * result
    return jnp.clip(result, min=-bound, max=bound).astype(kind)


def setup_inputs(seed: int = 0, part: int = 0) -> dict:
    key_list = jax.random.split(jax.random.key(seed), 14)
    part_keys = jax.random.split(jax.random.fold_in(key_list[13], part), 14)
    hidden = gaussian(part_keys[0], (REQUESTS, MODEL_WIDTH), 1.0, 6.0, ((0, 4),))
    input_norm_gain = jnp.clip(1.0 + 0.1 * jax.random.normal(key_list[1], (MODEL_WIDTH,), jnp.float32), 0.5, 1.5).astype(jnp.bfloat16)
    request_adapter = draw_request_adapter(jax.random.fold_in(jax.random.fold_in(key_list[13], part), 71), part)
    cache_fill_length = draw_cache_fill_length(jax.random.fold_in(jax.random.fold_in(key_list[13], part), 71), part)
    query_weight = gaussian(key_list[4], (MODEL_WIDTH, QUERY_HEAD_COUNT * HEAD_WIDTH), MODEL_WIDTH ** -0.5, 0.0625, ((0, 4), (1, 4)))
    key_weight = gaussian(key_list[5], (MODEL_WIDTH, KEY_VALUE_HEADS * HEAD_WIDTH), MODEL_WIDTH ** -0.5, 0.0625, ((0, 4), (1, 4)))
    value_weight = gaussian(key_list[6], (MODEL_WIDTH, KEY_VALUE_HEADS * HEAD_WIDTH), MODEL_WIDTH ** -0.5, 0.0625, ((0, 4), (1, 4)))
    output_weight = gaussian(key_list[7], (QUERY_HEAD_COUNT * HEAD_WIDTH, MODEL_WIDTH), (QUERY_HEAD_COUNT * HEAD_WIDTH) ** -0.5, 0.0625, ((0, 4), (1, 4)))
    down_weight_all = gaussian(key_list[8], (MODEL_WIDTH, ADAPTER_COUNT * 2 * ADAPTER_RANK), MODEL_WIDTH ** -0.5, 0.0625, ((0, 4), (1, 4)))
    query_up_weight = gaussian(key_list[9], (ADAPTER_COUNT * ADAPTER_RANK, QUERY_HEAD_COUNT * HEAD_WIDTH), ADAPTER_RANK ** -0.5, 1.5, ((0, 4), (1, 4)))
    value_up_weight = gaussian(key_list[10], (ADAPTER_COUNT * ADAPTER_RANK, KEY_VALUE_HEADS * HEAD_WIDTH), ADAPTER_RANK ** -0.5, 1.5, ((0, 4), (1, 4)))
    rotated_key_cache = draw_rotated_key_cache(jax.random.fold_in(jax.random.fold_in(key_list[13], part), 71), part)
    stored_value_cache = gaussian(part_keys[12], (REQUESTS, CTX, KEY_VALUE_HEADS * HEAD_WIDTH), 1.0, 6.0, ((0, 4), (2, 4)))
    return {"hidden": hidden, "input_norm_gain": input_norm_gain, "request_adapter": request_adapter, "cache_fill_length": cache_fill_length, "query_weight": query_weight, "key_weight": key_weight, "value_weight": value_weight, "output_weight": output_weight, "down_weight_all": down_weight_all, "query_up_weight": query_up_weight, "value_up_weight": value_up_weight, "rotated_key_cache": rotated_key_cache, "stored_value_cache": stored_value_cache}


ADAPTER_SCALE = 2.0
EPSILON = 1e-05
ROPE_BASE = 500000.0

def rotary(vectors, positions):
    count_rows = vectors.shape[0]
    split_heads = vectors.reshape(count_rows, -1, HEAD_WIDTH)
    halfway = HEAD_WIDTH // 2
    frequency = ROPE_BASE ** (-2.0 * jnp.arange(halfway, dtype=jnp.float32) / HEAD_WIDTH)
    angles = positions.astype(jnp.float32)[:, None] * frequency[None, :]
    cosine = jnp.cos(angles)[:, None, :]
    sine_part = jnp.sin(angles)[:, None, :]
    leading = split_heads[..., :halfway]
    trailing = split_heads[..., halfway:]
    turned = jnp.concatenate([leading * cosine - trailing * sine_part, trailing * cosine + leading * sine_part], axis=-1)
    return turned.reshape(count_rows, -1)

def attend_one(operands):
    query_row, key_fresh, value_fresh, cached_keys, cached_values, length = operands
    groups = QUERY_HEAD_COUNT // KEY_VALUE_HEADS
    score_scale = HEAD_WIDTH ** (-0.5)
    query_heads = query_row.astype(jnp.float32).reshape(KEY_VALUE_HEADS, groups, HEAD_WIDTH)
    key_heads = cached_keys.astype(jnp.float32).reshape(CTX, KEY_VALUE_HEADS, HEAD_WIDTH)
    value_heads = cached_values.astype(jnp.float32).reshape(CTX, KEY_VALUE_HEADS, HEAD_WIDTH)
    scores = jnp.einsum('kgd,ckd->kgc', query_heads, key_heads) * score_scale
    own_score = jnp.einsum('kgd,kd->kg', query_heads, key_fresh.astype(jnp.float32).reshape(KEY_VALUE_HEADS, HEAD_WIDTH)) * score_scale
    in_cache = jnp.arange(CTX, dtype=jnp.int32) < length
    masked = jnp.where(in_cache[None, None, :], scores, -1e+30)
    row_max = jnp.maximum(lax.optimization_barrier(jnp.max(masked, axis=-1)), own_score)
    exp_terms = jnp.where(in_cache[None, None, :], jnp.exp(masked - row_max[..., None]), 0.0)
    own_exp = jnp.exp(own_score - row_max)
    denominator = lax.optimization_barrier(jnp.sum(exp_terms, axis=-1)) + own_exp
    weights_low = (exp_terms / denominator[..., None]).astype(jnp.bfloat16)
    own_low = (own_exp / denominator).astype(jnp.bfloat16)
    mixed_heads = jnp.einsum('kgc,ckd->kgd', weights_low.astype(jnp.float32), value_heads)
    mixed_heads = mixed_heads + own_low.astype(jnp.float32)[..., None] * value_fresh.astype(jnp.float32).reshape(KEY_VALUE_HEADS, 1, HEAD_WIDTH)
    return mixed_heads.reshape(-1).astype(jnp.bfloat16)

def reference(hidden, input_norm_gain, request_adapter, cache_fill_length, query_weight, key_weight, value_weight, output_weight, down_weight_all, query_up_weight, value_up_weight, rotated_key_cache, stored_value_cache):
    widened = hidden.astype(jnp.float32)
    inverse = lax.rsqrt(lax.optimization_barrier(jnp.mean(widened * widened, axis=-1, keepdims=True)) + EPSILON)
    normalized_input = (widened * inverse * input_norm_gain.astype(jnp.float32)[None, :]).astype(jnp.bfloat16)
    query_matrix_rows = jnp.dot(normalized_input, query_weight, preferred_element_type=jnp.float32)
    key_rows = jnp.dot(normalized_input, key_weight, preferred_element_type=jnp.float32)
    value_matrix_rows = jnp.dot(normalized_input, value_weight, preferred_element_type=jnp.float32)
    down_projected = jnp.dot(normalized_input, down_weight_all, preferred_element_type=jnp.float32)
    column_owner = jnp.arange(down_projected.shape[1], dtype=jnp.int32) // (2 * ADAPTER_RANK)
    chosen = jnp.where(column_owner[None, :] == request_adapter[:, None], down_projected, 0.0).astype(jnp.bfloat16)
    split_rank = chosen.reshape(REQUESTS, ADAPTER_COUNT, 2 * ADAPTER_RANK)
    query_down_part = split_rank[:, :, :ADAPTER_RANK].reshape(REQUESTS, ADAPTER_COUNT * ADAPTER_RANK)
    value_down_part = split_rank[:, :, ADAPTER_RANK:].reshape(REQUESTS, ADAPTER_COUNT * ADAPTER_RANK)
    query_matrix_rows = query_matrix_rows + ADAPTER_SCALE * jnp.dot(query_down_part, query_up_weight, preferred_element_type=jnp.float32)
    value_matrix_rows = value_matrix_rows + ADAPTER_SCALE * jnp.dot(value_down_part, value_up_weight, preferred_element_type=jnp.float32)
    rotated_query = rotary(query_matrix_rows, cache_fill_length).astype(jnp.bfloat16)
    new_key = rotary(key_rows, cache_fill_length).astype(jnp.bfloat16)
    new_value = value_matrix_rows.astype(jnp.bfloat16)
    context = lax.map(attend_one, (rotated_query, new_key, new_value, rotated_key_cache, stored_value_cache, cache_fill_length))
    projected = jnp.dot(context, output_weight, preferred_element_type=jnp.float32)
    layer_out = (widened + projected).astype(jnp.bfloat16)
    return (layer_out, new_key, new_value)
```

```python
import functools

import jax
import jax.numpy as jnp
import numpy as np
from jax import lax
from jax.experimental import pallas as pl
from jax.experimental.pallas import tpu as pltpu
from jax.sharding import PartitionSpec as P

QUERY_HEAD_COUNT = 64
KEY_VALUE_HEADS = 8
HEAD_WIDTH = 128
ADAPTER_RANK = 16
ADAPTER_SCALE = 2.0
EPSILON = 1e-05
ROPE_BASE = 500000.0
MESH = pl.DeviceIdType.MESH
F32 = jnp.float32
BF16 = jnp.bfloat16
GROUPS = QUERY_HEAD_COUNT // KEY_VALUE_HEADS
REQ_STEP = 8


def dot(a, b):
    return jnp.dot(a, b, preferred_element_type=F32)


def start_remote(src, dst, send, recv, axis, index):
    copy = pltpu.make_async_remote_copy(
        src_ref=src, dst_ref=dst, send_sem=send, recv_sem=recv,
        device_id={axis: index}, device_id_type=MESH,
    )
    copy.start()
    return copy


def kernel(
    n, n_tp,
    hid_h, gain, ids_row, fill, fill_row, freq,
    qw_h, kw_h, vw_h, ow_h, dw_h, qu_h, vu_h, kc_h, vc_h,
    out, nk_out, nv_out,
    hid, qw, kw, vw, ow, dw, qu, vu, kc, vc,
    wide_gain, normed, route, rin, xin, xnorm, inv, shr, shr_in, tsend, term, rs, rq3, nk3, nv3, ctx3, ctx,
    osend, oterm, opair, osum, oown, ors,
    hid_sem, load_sem, route_s, route_r, x_s, x_r, pair_s, pair_r, inv_s, inv_r, shr_s, shr_r, rs_s, rs_r,
    ctx_s, ctx_r, out_s, out_r, far_s, far_r,
):
    a = lax.axis_index("ada")
    t = lax.axis_index("tp")
    core = lax.rem(t, 2)
    partner = t + 1 - 2 * core
    rows, model = hid.shape
    cap = route.shape[1]
    t_width = dw.shape[0]
    s_width = xin.shape[1]
    half = s_width // 2
    q_width, kv_width = qw.shape[1], kw.shape[1]
    share = oown.shape[0]
    chips = n_tp // 2
    chip = t // 2
    ranks2 = dw.shape[1]
    held = ranks2 // (2 * ADAPTER_RANK)

    hid_load = pltpu.make_async_copy(hid_h, hid, hid_sem)
    hid_load.start()
    loads = [
        pltpu.make_async_copy(src, dst, load_sem.at[i])
        for i, (src, dst) in enumerate(
            [(dw_h, dw), (qu_h, qu), (vu_h, vu), (kw_h, kw), (vw_h, vw), (qw_h, qw), (kc_h, kc), (vc_h, vc), (ow_h, ow)]
        )
    ]

    barrier = pltpu.get_barrier_semaphore()
    for d in range(1, n):
        pl.semaphore_signal(barrier, inc=1, device_id={"ada": lax.rem(a + d, n)}, device_id_type=MESH)
    for d in range(1, n_tp):
        pl.semaphore_signal(barrier, inc=1, device_id={"tp": lax.rem(t + d, n_tp)}, device_id_type=MESH)

    for load in loads:
        load.start()
    wide_gain[...] = gain[...].astype(F32)
    diagonal = lax.broadcasted_iota(jnp.int32, (rows, 128), 0) == lax.broadcasted_iota(jnp.int32, (rows, 128), 1)
    square = diagonal[:, :rows]

    def to_column(row):
        return jnp.sum(jnp.where(square, row, 0.0), axis=-1, keepdims=True)

    row_id = ids_row[...]
    col_id = to_column(row_id.astype(F32)).astype(jnp.int32)
    angles = to_column(fill_row[...].astype(F32)) * freq[...]
    cos_v, sin_v = jnp.cos(angles), jnp.sin(angles)
    sin_v = jnp.where(lax.broadcasted_iota(jnp.int32, sin_v.shape, 1) < HEAD_WIDTH // 2, -sin_v, sin_v)

    hid_load.wait()
    my_half = pl.ds(pl.multiple_of(core * half, 128), half)
    my_rows = pl.ds(pl.multiple_of(a * rows, rows), rows)
    pl.semaphore_wait(barrier, n - 1 + n_tp - 1)
    x_copies = []
    for d in range(1, n):
        to = lax.rem(a + d, n)
        x_copies.append(
            start_remote(
                hid.at[:, pl.ds(pl.multiple_of(to * s_width + core * half, 128), half)],
                xin.at[my_rows, my_half], x_s.at[d - 1], x_r.at[d - 1], "ada", to,
            )
        )

    step = 128
    squares = jnp.zeros((rows, step), F32)
    for c in range(0, model, step):
        wide = hid[:, c : c + step].astype(F32)
        squares = squares + wide * wide
    squares = jnp.sum(squares, axis=-1, keepdims=True)
    inverse = lax.rsqrt(squares / model + EPSILON)
    inv[a] = jnp.broadcast_to(
        jnp.sum(jnp.where(diagonal, inverse, 0.0), axis=0, keepdims=True), (8, 128)
    )
    inv_copies = []
    for d in range(1, n):
        to = lax.rem(a + d, n)
        inv_copies.append(start_remote(inv.at[a], inv.at[a], inv_s.at[d - 1], inv_r.at[d - 1], "ada", to))
    for c in range(0, model, step):
        wide = hid[:, c : c + step].astype(F32)
        normed[:, c : c + step] = (wide * inverse * wide_gain[c // step : c // step + 1, :]).astype(BF16)

    owner_row, owner_col = jnp.zeros_like(row_id), jnp.zeros_like(col_id)
    for o in range(1, n):
        owner_row = owner_row + (row_id >= o * held).astype(jnp.int32)
        owner_col = owner_col + (col_id >= o * held).astype(jnp.int32)
    before = lax.broadcasted_iota(jnp.int32, (rows, rows), 0) < lax.broadcasted_iota(jnp.int32, (rows, rows), 1)
    slot_row = jnp.sum(
        jnp.where((owner_col == owner_row) & before, 1.0, 0.0), axis=0, keepdims=True
    ).astype(jnp.int32)
    target = owner_row * cap + slot_row
    picker = jnp.where(
        lax.broadcasted_iota(jnp.int32, (n * cap, rows), 0) == target, 1.0, 0.0
    ).astype(BF16)
    first_col = (col_id - owner_col * held) * (2 * ADAPTER_RANK)
    lane = lax.broadcasted_iota(jnp.int32, (rows, ranks2), 1)
    colmask = jnp.where((lane >= first_col) & (lane < first_col + 2 * ADAPTER_RANK), 1.0, 0.0).astype(BF16)
    eye = jnp.where(diagonal, 1.0, 0.0).astype(BF16)
    mine = normed[:, pl.ds(pl.multiple_of(t * t_width, 128), t_width)]
    route[:, :, 0:t_width] = dot(picker, mine).astype(BF16).reshape(n, cap, t_width)
    route[:, :, t_width : t_width + ranks2] = dot(picker, colmask).astype(BF16).reshape(n, cap, ranks2)
    route[:, :, t_width + ranks2 :] = dot(picker, eye).astype(BF16).reshape(n, cap, 128)
    rin[a] = route[a]
    xin[my_rows, :] = hid[:, pl.ds(pl.multiple_of(a * s_width, 128), s_width)]

    pending = []
    for d in range(1, n):
        to = lax.rem(a + d, n)
        pending.append(start_remote(route.at[to], rin.at[a], route_s.at[d - 1], route_r.at[d - 1], "ada", to))

    pair_copies = []
    for d in range(1, n):
        source = lax.rem(a + n - d, n)
        x_copies[d - 1].wait_recv()
        region = xin.at[pl.ds(pl.multiple_of(source * rows, rows), rows), my_half]
        pair_copies.append(start_remote(region, region, pair_s.at[d - 1], pair_r.at[d - 1], "tp", partner))
    for copy in inv_copies + pair_copies:
        copy.wait_recv()
    for s in range(n):
        column = jnp.sum(jnp.where(diagonal, inv[s, 0:1, :], 0.0), axis=-1, keepdims=True)
        block = slice(s * rows, (s + 1) * rows)
        for c in range(0, s_width, step):
            gains = wide_gain[pl.ds(a * (s_width // step) + c // step, 1), :]
            xnorm[block, c : c + step] = (xin[block, c : c + step].astype(F32) * column * gains).astype(BF16)
    for load in loads[3:6]:
        load.wait()

    rs_copies = []

    def give(value, at, width, index):
        term[:, at : at + width] = value
        tsend[:, at : at + width] = value.astype(BF16)
        for d in range(1, n):
            to = lax.rem(a + d, n)
            rs_copies.append(
                start_remote(
                    tsend.at[pl.ds(pl.multiple_of(to * rows, rows), rows), pl.ds(at, width)],
                    rs.at[d - 1, :, pl.ds(at, width)], rs_s.at[index, d - 1], rs_r.at[index, d - 1], "ada", to,
                )
            )

    x = xnorm[...]
    give(dot(x, kw[...]), q_width, kv_width, 0)

    for load in loads[:3]:
        load.wait()
    for copy in pending:
        copy.wait_recv()
    shr[...] = dot(rin[:, :, 0:t_width].reshape(n * cap, t_width), dw[...])
    shr_copies = []
    for d in range(1, n_tp):
        to = lax.rem(t + d, n_tp)
        shr_copies.append(start_remote(shr, shr_in.at[d - 1], shr_s.at[d - 1], shr_r.at[d - 1], "tp", to))
    for copy in shr_copies:
        copy.wait_recv()
    total = shr[...]
    for d in range(1, n_tp):
        total = total + shr_in[d - 1]
    mask = rin[:, :, t_width : t_width + ranks2].reshape(n * cap, ranks2).astype(F32)
    chosen = (jnp.where(mask > 0.5, total, 0.0).astype(BF16).astype(F32) * ADAPTER_SCALE).astype(BF16)
    ups = []
    for offset in (0, ADAPTER_RANK):
        narrow = held * ADAPTER_RANK
        r_i = lax.broadcasted_iota(jnp.int32, (ranks2, narrow), 0)
        c_i = lax.broadcasted_iota(jnp.int32, (ranks2, narrow), 1)
        want = c_i + (c_i // ADAPTER_RANK) * ADAPTER_RANK + offset
        moved = dot(chosen, jnp.where(r_i == want, 1.0, 0.0).astype(BF16)).astype(BF16)
        placed = []
        for s in range(n):
            where_to = rin[s, :, t_width + ranks2 :]
            spread = lax.dot_general(
                where_to, moved[s * cap : (s + 1) * cap], (((0,), (0,)), ((), ())), preferred_element_type=F32
            )
            placed.append(spread[:rows])
        ups.append(jnp.concatenate(placed, axis=0).astype(BF16))

    give(dot(x, vw[...]) + dot(ups[1], vu[...]), q_width + kv_width, kv_width, 1)
    q_step = min(512, q_width)
    for i in range(q_width // q_step):
        at = i * q_step
        give(
            dot(x, qw[:, at : at + q_step]) + dot(ups[0], qu[:, at : at + q_step]), at, q_step, 2 + i
        )

    def summed(at, width):
        value = term[my_rows, at : at + width]
        for d in range(1, n):
            value = value + rs[d - 1, :, at : at + width].astype(F32)
        return value

    def turn(value):
        return (value * cos_v + pltpu.roll(value, HEAD_WIDTH // 2, 1) * sin_v).astype(BF16)

    def arrived(index):
        for copy in rs_copies[index * (n - 1) : (index + 1) * (n - 1)]:
            copy.wait_recv()

    kv_heads = kv_width // HEAD_WIDTH
    arrived(0)
    for h in range(kv_heads):
        cols = slice(h * HEAD_WIDTH, (h + 1) * HEAD_WIDTH)
        key = turn(summed(q_width + h * HEAD_WIDTH, HEAD_WIDTH))
        nk_out[:, cols] = key
        nk3[:, h, :] = key.astype(F32)
    arrived(1)
    for h in range(kv_heads):
        cols = slice(h * HEAD_WIDTH, (h + 1) * HEAD_WIDTH)
        fresh = summed(q_width + kv_width + h * HEAD_WIDTH, HEAD_WIDTH).astype(BF16)
        nv_out[:, cols] = fresh
        nv3[:, h, :] = fresh.astype(F32)
    score_scale = HEAD_WIDTH ** (-0.5)

    def attend(g, first):
        score_list, own_list, fill_list, val_list = [], [], [], []
        for j in range(REQ_STEP):
            r = first + j
            q = rq3[r, g * GROUPS : (g + 1) * GROUPS, :]
            keys = kc[r, :, g * HEAD_WIDTH : (g + 1) * HEAD_WIDTH]
            score_list.append(
                lax.dot_general(q.astype(BF16), keys, (((1,), (1,)), ((), ())), preferred_element_type=F32)
            )
            own_list.append(jnp.sum(q * nk3[r, g : g + 1, :], axis=-1, keepdims=True))
            val_list.append(jnp.broadcast_to(nv3[r, g : g + 1, :], (GROUPS, HEAD_WIDTH)))
            fill_list.append(jnp.full((GROUPS, 1), fill[r], jnp.int32))
        scores = jnp.concatenate(score_list, axis=0) * score_scale
        own = jnp.concatenate(own_list, axis=0) * score_scale
        lengths = jnp.concatenate(fill_list, axis=0)
        inside = lax.broadcasted_iota(jnp.int32, scores.shape, 1) < lengths
        masked = jnp.where(inside, scores, -1e30)
        top = jnp.maximum(jnp.max(masked, axis=-1, keepdims=True), own)
        terms = jnp.where(inside, jnp.exp(masked - top), 0.0)
        own_exp = jnp.exp(own - top)
        scale = 1.0 / (jnp.sum(terms, axis=-1, keepdims=True) + own_exp)
        low = (terms * scale).astype(BF16)
        own_part = (own_exp * scale).astype(BF16).astype(F32) * jnp.concatenate(val_list, axis=0)
        for j in range(REQ_STEP):
            r = first + j
            values = vc[r, :, g * HEAD_WIDTH : (g + 1) * HEAD_WIDTH]
            b = slice(j * GROUPS, (j + 1) * GROUPS)
            ctx3[r, g * GROUPS : (g + 1) * GROUPS, :] = dot(low[b], values) + own_part[b]

    ctx_copies = []
    turned = 0
    for g in range(kv_heads):
        while turned * HEAD_WIDTH < (g + 1) * GROUPS * HEAD_WIDTH:
            if turned * HEAD_WIDTH % q_step == 0:
                arrived(2 + turned * HEAD_WIDTH // q_step)
            rq3[:, turned, :] = turn(summed(turned * HEAD_WIDTH, HEAD_WIDTH)).astype(F32)
            turned += 1
        if g == 0:
            for load in loads[6:8]:
                load.wait()

        @pl.loop(0, rows // REQ_STEP)
        def _(i):
            attend(g, i * REQ_STEP)

        for h in range(g * GROUPS, (g + 1) * GROUPS):
            ctx[my_rows, h * HEAD_WIDTH : (h + 1) * HEAD_WIDTH] = ctx3[:, h, :].astype(BF16)
        here = ctx.at[my_rows, pl.ds(g * GROUPS * HEAD_WIDTH, GROUPS * HEAD_WIDTH)]
        for d in range(1, n):
            to = lax.rem(a + d, n)
            ctx_copies.append(start_remote(here, here, ctx_s.at[g, d - 1], ctx_r.at[g, d - 1], "ada", to))
    loads[8].wait()
    for copy in ctx_copies:
        copy.wait_recv()

    o_step = min(512, s_width)
    out_copies = []
    every = ctx[...]
    for i in range(s_width // o_step):
        at = i * o_step
        value = dot(every, ow[:, at : at + o_step])
        oterm[:, at : at + o_step] = value
        osend[:, at : at + o_step] = value.astype(BF16)
        for j in range(chips):
            out_copies.append(
                start_remote(
                    osend.at[pl.ds(pl.multiple_of((2 * j + 1 - core) * share, share), share), pl.ds(at, o_step)],
                    opair.at[j, :, pl.ds(at, o_step)], out_s.at[i, j], out_r.at[i, j], "tp", partner,
                )
            )

    far_copies = []
    for i in range(s_width // o_step):
        cols = slice(i * o_step, (i + 1) * o_step)
        for copy in out_copies[i * chips : (i + 1) * chips]:
            copy.wait_recv()
        for e in range(1, chips):
            to = lax.rem(chip + e, chips)
            there = pl.ds(pl.multiple_of((2 * to + core) * share, share), share)
            osum[e - 1, :, cols] = (oterm[there, cols] + opair[to, :, cols].astype(F32)).astype(BF16)
            far_copies.append(
                start_remote(
                    osum.at[e - 1, :, pl.ds(i * o_step, o_step)], ors.at[e - 1, :, pl.ds(i * o_step, o_step)],
                    far_s.at[i, e - 1], far_r.at[i, e - 1], "tp", 2 * to + core,
                )
            )

    out_rows = pl.ds(pl.multiple_of(t * share, share), share)
    for i in range(s_width // o_step):
        cols = slice(i * o_step, (i + 1) * o_step)
        oown[:, cols] = (
            xin[out_rows, cols].astype(F32) + (oterm[out_rows, cols] + opair[chip, :, cols].astype(F32))
        )
    for i in range(s_width // o_step):
        cols = slice(i * o_step, (i + 1) * o_step)
        for copy in far_copies[i * (chips - 1) : (i + 1) * (chips - 1)]:
            copy.wait_recv()
        value = oown[:, cols]
        for e in range(1, chips):
            value = value + ors[e - 1, :, cols].astype(F32)
        out[:, cols] = value.astype(BF16)

    for copy in (
        pending + x_copies + inv_copies + shr_copies + pair_copies + rs_copies + ctx_copies + out_copies + far_copies
    ):
        copy.wait_send()


def on_device(
    n, n_tp, hidden, input_norm_gain, request_adapter, cache_fill_length, query_weight, key_weight,
    value_weight, output_weight, down_weight_all, query_up_weight, value_up_weight,
    rotated_key_cache, stored_value_cache,
):
    rows, model = hidden.shape
    q_width, kv_width = query_weight.shape[1], key_weight.shape[1]
    s_width, t_width = query_weight.shape[0], down_weight_all.shape[0]
    ranks2 = down_weight_all.shape[1]
    cap = max(2, (2 * rows + n - 1) // n)
    cap = (cap + 15) // 16 * 16
    share = n * rows // n_tp
    chips = n_tp // 2
    total = q_width + 2 * kv_width
    kv_heads, heads = kv_width // HEAD_WIDTH, q_width // HEAD_WIDTH
    halfway = HEAD_WIDTH // 2
    frequency = np.float32(ROPE_BASE) ** (np.float32(-2.0) * np.arange(halfway, dtype=np.float32) / np.float32(HEAD_WIDTH))
    frequency = jnp.asarray(np.concatenate([frequency, frequency])[None, :])
    big = [query_weight, key_weight, value_weight, output_weight, down_weight_all, query_up_weight,
           value_up_weight, rotated_key_cache, stored_value_cache]
    chunks = 2 + q_width // min(512, q_width)
    o_chunks = s_width // min(512, s_width)
    vmem = pl.BlockSpec(memory_space=pltpu.VMEM)
    dma = pltpu.SemaphoreType.DMA
    v = pltpu.VMEM
    lanes = 128
    scratch = [v(hidden.shape, hidden.dtype)] + [v(w.shape, w.dtype) for w in big] + [
        v((model // lanes, lanes), F32),
        v((rows, model), BF16),
        v((n, cap, t_width + ranks2 + 128), BF16),
        v((n, cap, t_width + ranks2 + 128), BF16),
        v((n * rows, s_width), BF16),
        v((n * rows, s_width), BF16),
        v((n, 8, 128), F32),
        v((n * cap, ranks2), F32),
        v((n_tp - 1, n * cap, ranks2), F32),
        v((n * rows, total), BF16),
        v((n * rows, total), F32),
        v((n - 1, rows, total), BF16),
        v((rows, heads, HEAD_WIDTH), F32),
        v((rows, kv_heads, HEAD_WIDTH), F32),
        v((rows, kv_heads, HEAD_WIDTH), F32),
        v((rows, heads, HEAD_WIDTH), F32),
        v((n * rows, q_width), BF16),
        v((n * rows, s_width), BF16),
        v((n * rows, s_width), F32),
        v((chips, share, s_width), BF16),
        v((chips - 1, share, s_width), BF16),
        v((share, s_width), F32),
        v((chips - 1, share, s_width), BF16),
        dma, dma((9,)),
        dma((n - 1,)), dma((n - 1,)),
        dma((n - 1,)), dma((n - 1,)),
        dma((n - 1,)), dma((n - 1,)),
        dma((n - 1,)), dma((n - 1,)),
        dma((n_tp - 1,)), dma((n_tp - 1,)),
        dma((chunks, n - 1)), dma((chunks, n - 1)),
        dma((kv_heads, n - 1)), dma((kv_heads, n - 1)),
        dma((o_chunks, chips)), dma((o_chunks, chips)),
        dma((o_chunks, chips - 1)), dma((o_chunks, chips - 1)),
    ]
    shapes = [((share, s_width), BF16), ((rows, kv_width), BF16), ((rows, kv_width), BF16)]
    held = pl.pallas_call(
        functools.partial(kernel, n, n_tp),
        out_shape=[pltpu.VMEM(*one) for one in shapes],
        in_specs=[pl.BlockSpec(memory_space=pl.ANY)] + [vmem] * 2 + [pl.BlockSpec(memory_space=pltpu.SMEM)] + [vmem] * 2
        + [pl.BlockSpec(memory_space=pl.ANY)] * 9,
        out_specs=[vmem] * 3,
        scratch_shapes=scratch,
        compiler_params=pltpu.CompilerParams(
            collective_id=0, has_side_effects=True, vmem_limit_bytes=62 * 1024 * 1024
        ),
    )(
        hidden, input_norm_gain.reshape(model // lanes, lanes), request_adapter[None, :],
        cache_fill_length, cache_fill_length[None, :], frequency, *big,
    )
    return tuple(held)


def solution(mesh):
    return jax.shard_map(
        functools.partial(on_device, mesh.shape["ada"], mesh.shape["tp"]),
        mesh=mesh,
        in_specs=(
            P(("rep", "ada"), None),
            P(),
            P(("rep", "ada")),
            P(("rep", "ada")),
            P("ada", "tp"),
            P("ada", "tp"),
            P("ada", "tp"),
            P("tp", "ada"),
            P("tp", "ada"),
            P("ada", "tp"),
            P("ada", "tp"),
            P(("rep", "ada"), None, "tp"),
            P(("rep", "ada"), None, "tp"),
        ),
        out_specs=(P(("rep", "tp"), "ada"), P(("rep", "ada"), "tp"), P(("rep", "ada"), "tp")),
        check_vma=False,
    )
```

```python
import functools

import jax
import jax.numpy as jnp
import numpy as np
from jax import lax
from jax.experimental import pallas as pl
from jax.experimental.pallas import tpu as pltpu
from jax.sharding import PartitionSpec as P

QUERY_HEAD_COUNT = 64
KEY_VALUE_HEADS = 8
HEAD_WIDTH = 128
ADAPTER_RANK = 16
ADAPTER_SCALE = 2.0
EPSILON = 1e-05
ROPE_BASE = 500000.0
MESH = pl.DeviceIdType.MESH
F32 = jnp.float32
BF16 = jnp.bfloat16
GROUPS = QUERY_HEAD_COUNT // KEY_VALUE_HEADS
REQ_STEP = 8


def dot(a, b):
    return jnp.dot(a, b, preferred_element_type=F32)


def remote(src, dst, send, recv, target):
    return pltpu.make_async_remote_copy(
        src_ref=src, dst_ref=dst, send_sem=send, recv_sem=recv, device_id=target, device_id_type=MESH
    )


def kernel(
    n, n_tp,
    hid_h, gain_h, ids_h, fill_h, freq_h, qw_h, kw_h, vw_h, ow_h, dw_h, qu_h, vu_h, kc_h, vc_h,
    out, nk_out, nv_out,
    hid, qw, kw, vw, ow, dw, qu, vu, kc, vc,
    gain, ids_row, fill_row, freq, fill, wide_gain, normed, meta, route, rin, xin, xnorm, shr, shr_in, tsend, term, rs, rq3, nk3, nv3, ctx3, ctx,
    osend, oterm, opair, osum, oown, ors,
    hid_sem, small_sem, load_sem, meta_s, meta_r, route_s, route_r, x_s, x_r, pair_s, pair_r, shr_s, shr_r, rs_s, rs_r,
    ctx_s, ctx_r, out_s, out_r, far_s, far_r,
):
    a = lax.axis_index("ada")
    t = lax.axis_index("tp")
    core = lax.rem(t, 2)
    partner = t + 1 - 2 * core
    rows, model = hid.shape
    cap = route.shape[1]
    t_width, ranks2 = dw.shape
    s_width = xin.shape[1]
    half = s_width // 2
    q_width, kv_width = qw.shape[1], kw.shape[1]
    kv_heads = kv_width // HEAD_WIDTH
    share = oown.shape[0]
    chips = n_tp // 2
    chip = t // 2
    pair = 2 * ADAPTER_RANK
    held = ranks2 // pair
    step = 128
    relays = n > 3

    first = 1 - lax.div(a + n - 1, n)
    last = lax.div(a + 1, n)
    upper = lax.div(2 * a, n)
    is_end = jnp.logical_and(relays, jnp.logical_or(a == 0, a == n - 1))
    is_next = jnp.logical_and(relays, jnp.logical_or(a == 1, a == n - 2))
    end = (first + last) if relays else 0

    def peer(k):
        low = n - 1 - k
        low = low - lax.div(a - low + n, n)
        high = k + lax.div(k - a + n, n)
        return low + upper * (high - low)

    def block(index, size):
        return pl.ds(pl.multiple_of(index * size, size), size)

    def when(condition, action):
        if condition is True:
            action()
        elif condition is not False:
            pl.when(condition)(action)

    hid_load = pltpu.make_async_copy(hid_h, hid, hid_sem)
    hid_load.start()
    small_loads = [
        pltpu.make_async_copy(src, dst, small_sem.at[i])
        for i, (src, dst) in enumerate(
            [(gain_h, gain), (ids_h, ids_row), (fill_h, fill_row), (freq_h, freq), (fill_h, fill)]
        )
    ]
    for load in small_loads:
        load.start()
    barrier = pltpu.get_barrier_semaphore()
    for d in range(1, n):
        pl.semaphore_signal(barrier, inc=1, device_id={"ada": lax.rem(a + d, n)}, device_id_type=MESH)
    for d in range(1, n_tp):
        pl.semaphore_signal(barrier, inc=1, device_id={"tp": lax.rem(t + d, n_tp)}, device_id_type=MESH)
    loads = [
        pltpu.make_async_copy(src, dst, load_sem.at[i])
        for i, (src, dst) in enumerate(
            [(dw_h, dw), (qu_h, qu), (vu_h, vu), (kw_h, kw), (vw_h, vw), (qw_h, qw), (kc_h, kc), (vc_h, vc), (ow_h, ow)]
        )
    ]
    for load in loads:
        load.start()

    for load in small_loads:
        load.wait()
    wide_gain[...] = gain[...].astype(F32)
    diagonal = lax.broadcasted_iota(jnp.int32, (rows, 128), 0) == lax.broadcasted_iota(jnp.int32, (rows, 128), 1)
    square = diagonal[:, :rows]
    before = lax.broadcasted_iota(jnp.int32, (rows, rows), 0) < lax.broadcasted_iota(jnp.int32, (rows, rows), 1)

    def to_column(row):
        return jnp.sum(jnp.where(square, row, 0.0), axis=-1, keepdims=True)

    def to_row(column):
        return jnp.sum(jnp.where(diagonal, column, 0.0), axis=0, keepdims=True)

    row_id = ids_row[...].astype(F32)
    col_id = to_column(row_id)
    angles = to_column(fill_row[...].astype(F32)) * freq[...]
    cos_v, sin_v = jnp.cos(angles), jnp.sin(angles)
    sin_v = jnp.where(lax.broadcasted_iota(jnp.int32, sin_v.shape, 1) < HEAD_WIDTH // 2, -sin_v, sin_v)
    owner_row, owner_col = jnp.zeros_like(row_id), jnp.zeros_like(col_id)
    for o in range(1, n):
        owner_row = owner_row + (row_id >= o * held).astype(F32)
        owner_col = owner_col + (col_id >= o * held).astype(F32)
    slot_row = jnp.sum(jnp.where((owner_col == owner_row) & before, 1.0, 0.0), axis=0, keepdims=True)
    target = (owner_row * cap + slot_row).astype(jnp.int32)
    picker = jnp.where(
        lax.broadcasted_iota(jnp.int32, (n * cap, rows), 0) == target, 1.0, 0.0
    ).astype(BF16)
    if relays:
        @pl.when(is_end)
        def _():
            rs[peer(0), :, :q_width] = jnp.zeros((rows, q_width), rs.dtype)

    hid_load.wait()
    squares = jnp.zeros((rows, step), F32)
    for c in range(0, model, step):
        wide = hid[:, c : c + step].astype(F32)
        squares = squares + wide * wide
    inverse = lax.rsqrt(jnp.sum(squares, axis=-1, keepdims=True) / model + EPSILON)
    meta[a] = jnp.where(
        lax.broadcasted_iota(jnp.int32, (8, 128), 0) == 0, to_row(inverse), to_row(col_id)
    )
    for c in range(0, model, step):
        wide = hid[:, c : c + step].astype(F32)
        normed[:, c : c + step] = (wide * inverse * wide_gain[c // step : c // step + 1, :]).astype(BF16)
    route[...] = dot(picker, normed[:, block(t, t_width)]).astype(BF16).reshape(n, cap, t_width)
    rin[a] = route[a]
    my_rows = block(a, rows)
    my_half = block(core, half)
    xin[my_rows, :] = hid[:, block(a, s_width)]

    pl.semaphore_wait(barrier, n - 1 + n_tp - 1)
    sends = []

    def go(copy):
        copy.start()
        sends.append(copy)

    for k in range(n - 1):
        to = peer(k)
        go(remote(meta.at[a], meta.at[a], meta_s.at[k], meta_r.at[a], {"ada": to}))
    for k in range(n - 1):
        to = peer(k)
        go(remote(route.at[to], rin.at[a], route_s.at[k], route_r.at[a], {"ada": to}))
    for k in range(n - 1):
        to = peer(k)
        go(
            remote(
                hid.at[:, pl.ds(pl.multiple_of(to * s_width + core * half, 128), half)],
                xin.at[my_rows, my_half], x_s.at[k], x_r.at[a], {"ada": to},
            )
        )
    near_first = [peer(k) for k in reversed(range(n - 1))]

    def landed(dst, send, recv):
        remote(dst, dst, send, recv, {"ada": lax.rem(a + 1, n)}).wait_recv()

    for s in near_first:
        landed(meta.at[s], meta_s.at[0], meta_r.at[s])
    lane_cap = lax.broadcasted_iota(jnp.int32, (cap, ranks2), 1) // pair
    lane_rows = lax.broadcasted_iota(jnp.int32, (rows, ranks2), 1) // pair
    low_id = (a * held).astype(F32)
    places, slot_masks, id_cols, scales = [], [], [], []
    for s in range(n):
        ids_s = meta[s, 1:2, :rows]
        col_s = to_column(ids_s)
        here_row = (ids_s >= low_id) & (ids_s < low_id + held)
        here_col = (col_s >= low_id) & (col_s < low_id + held)
        slots = jnp.sum(jnp.where(here_col & before, 1.0, 0.0), axis=0, keepdims=True)
        chosen_slot = lax.broadcasted_iota(jnp.int32, (cap, rows), 0) == slots.astype(jnp.int32)
        slot_id = jnp.sum(jnp.where(chosen_slot & here_row, ids_s - low_id, 0.0), axis=-1, keepdims=True)
        slot_masks.append(lane_cap == slot_id.astype(jnp.int32))
        slot_col = to_column(slots).astype(jnp.int32)
        places.append(
            jnp.where((lax.broadcasted_iota(jnp.int32, (rows, cap), 1) == slot_col) & here_col, 1.0, 0.0).astype(BF16)
        )
        id_cols.append((col_s - low_id).astype(jnp.int32))
        scales.append(to_column(meta[s, 0:1, :rows]))
    row_ids = jnp.concatenate(id_cols, axis=0)

    loads[0].wait()
    for s in near_first:
        landed(rin.at[s], route_s.at[0], route_r.at[s])
    partial = dot(rin[...].reshape(n * cap, t_width), dw[...])
    for first_s in range(0, n, held):
        tile = jnp.zeros((cap, ranks2), F32)
        for s in range(first_s, min(n, first_s + held)):
            picked = jnp.where(slot_masks[s], partial[s * cap : (s + 1) * cap], 0.0)
            folded = picked
            for i in range(1, held):
                folded = folded + pltpu.roll(picked, i * pair, 1)
            tile = jnp.where(lane_cap == s - first_s, folded, tile)
        shr[first_s // held * cap : (first_s // held + 1) * cap, :] = tile
    for d in range(1, n_tp):
        to = lax.rem(t + d, n_tp)
        go(remote(shr, shr_in.at[d - 1], shr_s.at[d - 1], shr_r.at[d - 1], {"tp": to}))

    def x_region(s):
        return xin.at[block(s, rows), my_half]

    for s in near_first:
        landed(x_region(s), x_s.at[0], x_r.at[s])
        go(remote(x_region(s), x_region(s), pair_s.at[s], pair_r.at[s], {"tp": partner}))

    for copy in sends[-(n - 1) - (n_tp - 1) : -(n - 1)]:
        copy.wait_recv()
    total = shr[...]
    for d in range(1, n_tp):
        total = total + shr_in[d - 1]
    chosen = (total.astype(BF16).astype(F32) * ADAPTER_SCALE).astype(BF16)
    spread = []
    for s in range(n):
        mine = chosen[s // held * cap : (s // held + 1) * cap]
        spread.append(jnp.where(lane_rows == s % held, dot(places[s], mine), 0.0))
    spread = jnp.concatenate(spread, axis=0).astype(BF16)
    narrow = held * ADAPTER_RANK
    from_lane = lax.broadcasted_iota(jnp.int32, (ranks2, narrow), 0) % pair
    to_lane = lax.broadcasted_iota(jnp.int32, (ranks2, narrow), 1) % ADAPTER_RANK
    own_lane = lax.broadcasted_iota(jnp.int32, (n * rows, narrow), 1) // ADAPTER_RANK == row_ids
    ups = []
    for offset in (0, ADAPTER_RANK):
        moved = dot(spread, jnp.where(from_lane == to_lane + offset, 1.0, 0.0).astype(BF16))
        ups.append(jnp.where(own_lane, moved, 0.0).astype(BF16))

    for s in near_first:
        other = xin.at[block(s, rows), block(1 - core, half)]
        landed(other, pair_s.at[s], pair_r.at[s])
    for s in range(n):
        rows_s = slice(s * rows, (s + 1) * rows)
        for c in range(0, s_width, step):
            gains = wide_gain[pl.ds(a * (s_width // step) + c // step, 1), :]
            xnorm[rows_s, c : c + step] = (xin[rows_s, c : c + step].astype(F32) * scales[s] * gains).astype(BF16)
    for load in loads[1:6]:
        load.wait()

    spare = n
    beside = first + last * (n - 2)
    far_target = peer(0) + end * (beside - peer(0))
    far_slot = a + end * (spare - a)
    chunks = []

    def chunk_copy(index, k):
        at, width = chunks[index]
        cols = pl.ds(at, width)
        to = peer(k)
        target, slot = (far_target, far_slot) if k == 0 and index > 0 else (to, a)
        return remote(
            tsend.at[block(to, rows), cols], rs.at[slot, :, cols], rs_s.at[index, k], rs_r.at[index, slot],
            {"ada": target},
        )

    def give(value, at, width):
        index = len(chunks)
        chunks.append((at, width))
        term[:, at : at + width] = value
        tsend[:, at : at + width] = value.astype(BF16)

    def ship(index, k):
        direct = k > 0 or index == 0 or not relays
        when(True if direct else jnp.logical_not(is_next), lambda: chunk_copy(index, k).start())

    def relay(index):
        if not relays:
            return
        at, width = chunks[index]
        cols = pl.ds(at, width)

        @pl.when(is_next)
        def _():
            landed(rs.at[spare, :, cols], rs_s.at[index, 0], rs_r.at[index, spare])
            there = block(peer(0), rows)
            tsend[there, cols] = (term[there, cols] + rs[spare, :, cols].astype(F32)).astype(BF16)
            remote(
                tsend.at[there, cols], rs.at[a, :, cols], rs_s.at[index, 0], rs_r.at[index, a], {"ada": peer(0)}
            ).start()

    def arrived(index):
        at, width = chunks[index]
        cols = pl.ds(at, width)
        for k in reversed(range(n - 1)):
            s = peer(k)
            when(
                jnp.logical_not(is_end) if relays and k == 0 and index > 0 else True,
                lambda: landed(rs.at[s, :, cols], rs_s.at[index, 0], rs_r.at[index, s]),
            )

    x = xnorm[...]
    give(
        jnp.concatenate([dot(x, kw[...]), dot(x, vw[...]) + dot(ups[1], vu[...])], axis=1), q_width, 2 * kv_width
    )
    for k in range(n - 1):
        ship(0, k)
    wide_g = GROUPS * HEAD_WIDTH
    q_step = min(512, wide_g)
    per_g = wide_g // q_step
    for g in range(kv_heads):
        group = range(1 + g * per_g, 1 + (g + 1) * per_g)
        for index in group:
            at = (index - 1) * q_step
            give(dot(x, qw[:, at : at + q_step]) + dot(ups[0], qu[:, at : at + q_step]), at, q_step)
            if g == 0:
                ship(index, 0)
        if g == 0:
            for k in range(1, n - 1):
                for index in group:
                    ship(index, k)
    for index in range(1, 1 + per_g):
        relay(index)
    for g in range(1, kv_heads):
        for k in range(n - 1):
            for index in range(1 + g * per_g, 1 + (g + 1) * per_g):
                ship(index, k)

    def summed(at, width):
        value = term[my_rows, at : at + width]
        for k in range(n - 1):
            value = value + rs[peer(k), :, at : at + width].astype(F32)
        return value

    def turn(value):
        return (value * cos_v + pltpu.roll(value, HEAD_WIDTH // 2, 1) * sin_v).astype(BF16)

    arrived(0)
    for h in range(kv_heads):
        cols = slice(h * HEAD_WIDTH, (h + 1) * HEAD_WIDTH)
        key = turn(summed(q_width + h * HEAD_WIDTH, HEAD_WIDTH))
        nk_out[:, cols] = key
        nk3[:, h, :] = key.astype(F32)
    for h in range(kv_heads):
        cols = slice(h * HEAD_WIDTH, (h + 1) * HEAD_WIDTH)
        fresh = summed(q_width + kv_width + h * HEAD_WIDTH, HEAD_WIDTH).astype(BF16)
        nv_out[:, cols] = fresh
        nv3[:, h, :] = fresh.astype(F32)
    score_scale = HEAD_WIDTH ** (-0.5)

    def attend(g, start):
        score_list, own_list, fill_list, val_list = [], [], [], []
        for j in range(REQ_STEP):
            r = start + j
            q = rq3[r, g * GROUPS : (g + 1) * GROUPS, :]
            keys = kc[r, :, g * HEAD_WIDTH : (g + 1) * HEAD_WIDTH]
            score_list.append(
                lax.dot_general(q.astype(BF16), keys, (((1,), (1,)), ((), ())), preferred_element_type=F32)
            )
            own_list.append(jnp.sum(q * nk3[r, g : g + 1, :], axis=-1, keepdims=True))
            val_list.append(jnp.broadcast_to(nv3[r, g : g + 1, :], (GROUPS, HEAD_WIDTH)))
            fill_list.append(jnp.full((GROUPS, 1), fill[0, r], jnp.int32))
        scores = jnp.concatenate(score_list, axis=0) * score_scale
        own = jnp.concatenate(own_list, axis=0) * score_scale
        lengths = jnp.concatenate(fill_list, axis=0)
        inside = lax.broadcasted_iota(jnp.int32, scores.shape, 1) < lengths
        masked = jnp.where(inside, scores, -1e30)
        top = jnp.maximum(jnp.max(masked, axis=-1, keepdims=True), own)
        terms = jnp.where(inside, jnp.exp(masked - top), 0.0)
        own_exp = jnp.exp(own - top)
        scale = 1.0 / (jnp.sum(terms, axis=-1, keepdims=True) + own_exp)
        low = (terms * scale).astype(BF16)
        own_part = (own_exp * scale).astype(BF16).astype(F32) * jnp.concatenate(val_list, axis=0)
        for j in range(REQ_STEP):
            r = start + j
            values = vc[r, :, g * HEAD_WIDTH : (g + 1) * HEAD_WIDTH]
            b = slice(j * GROUPS, (j + 1) * GROUPS)
            ctx3[r, g * GROUPS : (g + 1) * GROUPS, :] = dot(low[b], values) + own_part[b]

    piece = min(16, rows)
    pieces = rows // piece

    def ctx_region(s, index):
        g, p = index // pieces, index % pieces
        return ctx.at[pl.ds(pl.multiple_of(s * rows + p * piece, piece), piece), pl.ds(g * wide_g, wide_g)]

    def ctx_copy(index, k):
        return remote(
            ctx_region(a, index), ctx_region(a, index), ctx_s.at[index, k], ctx_r.at[index, a], {"ada": peer(k)}
        )

    def pass_copy(index):
        s = peer(0)
        outward = lax.div(a, n - 2) * (n - 1)
        return remote(
            ctx_region(s, index), ctx_region(s, index), ctx_s.at[index, n - 1], ctx_r.at[index, s], {"ada": outward}
        )

    def ctx_landed(s, index):
        landed(ctx_region(s, index), ctx_s.at[index, 0], ctx_r.at[index, s])

    def pass_on(index):
        if not relays:
            return

        @pl.when(is_next)
        def _():
            ctx_landed(peer(0), index)
            pass_copy(index).start()

    def gathered(index):
        for k in reversed(range(n - 1)):
            s = peer(k)
            when(
                jnp.logical_not(is_next) if relays and k == 0 else True,
                lambda: ctx_landed(s, index),
            )

    turned = 0
    for g in range(kv_heads):
        for index in range(1 + g * per_g, 1 + (g + 1) * per_g):
            arrived(index)
        while turned < (g + 1) * GROUPS:
            rq3[:, turned, :] = turn(summed(turned * HEAD_WIDTH, HEAD_WIDTH)).astype(F32)
            turned += 1
        if g < kv_heads - 1:
            for index in range(1 + (g + 1) * per_g, 1 + (g + 2) * per_g):
                relay(index)
        if g == 0:
            for load in loads[6:8]:
                load.wait()
        for p in range(pieces):
            @pl.loop(0, piece // REQ_STEP)
            def _(i):
                attend(g, p * piece + i * REQ_STEP)

            own_rows = pl.ds(pl.multiple_of(a * rows + p * piece, piece), piece)
            for h in range(g * GROUPS, (g + 1) * GROUPS):
                ctx[own_rows, h * HEAD_WIDTH : (h + 1) * HEAD_WIDTH] = ctx3[
                    p * piece : (p + 1) * piece, h, :
                ].astype(BF16)
            index = g * pieces + p
            when(jnp.logical_not(is_end) if relays else True, lambda: ctx_copy(index, 0).start())
            for k in range(1, n - 1):
                ctx_copy(index, k).start()

    loads[8].wait()
    o_step = min(512, s_width)
    out_copies = []
    for g in range(kv_heads):
        for p in range(pieces):
            pass_on(g * pieces + p)
        for p in range(pieces):
            gathered(g * pieces + p)
        part = ctx[:, g * wide_g : (g + 1) * wide_g]
        for i in range(s_width // o_step):
            at = i * o_step
            value = dot(part, ow[g * wide_g : (g + 1) * wide_g, at : at + o_step])
            if g > 0:
                value = value + oterm[:, at : at + o_step]
            oterm[:, at : at + o_step] = value
            if g < kv_heads - 1:
                continue
            osend[:, at : at + o_step] = value.astype(BF16)
            for j in range(chips):
                out_copies.append(
                    remote(
                        osend.at[block(2 * j + 1 - core, share), pl.ds(at, o_step)],
                        opair.at[j, :, pl.ds(at, o_step)], out_s.at[i, j], out_r.at[i, j], {"tp": partner},
                    )
                )
                go(out_copies[-1])

    far_copies = []
    for i in range(s_width // o_step):
        cols = slice(i * o_step, (i + 1) * o_step)
        for copy in out_copies[i * chips : (i + 1) * chips]:
            copy.wait_recv()
        for e in range(1, chips):
            to = lax.rem(chip + e, chips)
            there = block(2 * to + core, share)
            osum[e - 1, :, cols] = (oterm[there, cols] + opair[to, :, cols].astype(F32)).astype(BF16)
            far_copies.append(
                remote(
                    osum.at[e - 1, :, pl.ds(i * o_step, o_step)], ors.at[e - 1, :, pl.ds(i * o_step, o_step)],
                    far_s.at[i, e - 1], far_r.at[i, e - 1], {"tp": 2 * to + core},
                )
            )
            go(far_copies[-1])

    out_rows = block(t, share)
    for i in range(s_width // o_step):
        cols = slice(i * o_step, (i + 1) * o_step)
        oown[:, cols] = (
            xin[out_rows, cols].astype(F32) + (oterm[out_rows, cols] + opair[chip, :, cols].astype(F32))
        )
    for i in range(s_width // o_step):
        cols = slice(i * o_step, (i + 1) * o_step)
        for copy in far_copies[i * (chips - 1) : (i + 1) * (chips - 1)]:
            copy.wait_recv()
        value = oown[:, cols]
        for e in range(1, chips):
            value = value + ors[e - 1, :, cols].astype(F32)
        out[:, cols] = value.astype(BF16)

    for copy in sends:
        copy.wait_send()
    for index in range(len(chunks)):
        for k in range(n - 1):
            chunk_copy(index, k).wait_send()
    for index in range(kv_heads * pieces):
        when(jnp.logical_not(is_end) if relays else True, lambda: ctx_copy(index, 0).wait_send())
        for k in range(1, n - 1):
            ctx_copy(index, k).wait_send()
        when(is_next if relays else False, lambda: pass_copy(index).wait_send())


def on_device(
    n, n_tp, hidden, input_norm_gain, request_adapter, cache_fill_length, query_weight, key_weight,
    value_weight, output_weight, down_weight_all, query_up_weight, value_up_weight,
    rotated_key_cache, stored_value_cache,
):
    rows, model = hidden.shape
    q_width, kv_width = query_weight.shape[1], key_weight.shape[1]
    s_width, t_width = query_weight.shape[0], down_weight_all.shape[0]
    ranks2 = down_weight_all.shape[1]
    cap = max(2, (2 * rows + n - 1) // n)
    cap = (cap + 15) // 16 * 16
    share = n * rows // n_tp
    chips = n_tp // 2
    total = q_width + 2 * kv_width
    kv_heads, heads = kv_width // HEAD_WIDTH, q_width // HEAD_WIDTH
    halfway = HEAD_WIDTH // 2
    frequency = np.float32(ROPE_BASE) ** (np.float32(-2.0) * np.arange(halfway, dtype=np.float32) / np.float32(HEAD_WIDTH))
    frequency = jnp.asarray(np.concatenate([frequency, frequency])[None, :])
    big = [query_weight, key_weight, value_weight, output_weight, down_weight_all, query_up_weight,
           value_up_weight, rotated_key_cache, stored_value_cache]
    chunks = 1 + q_width // min(512, GROUPS * HEAD_WIDTH)
    o_chunks = s_width // min(512, s_width)
    pieces = rows // min(16, rows)
    per_pack = ranks2 // (2 * ADAPTER_RANK)
    packs = (n + per_pack - 1) // per_pack
    vmem = pl.BlockSpec(memory_space=pltpu.VMEM)
    dma = pltpu.SemaphoreType.DMA
    v = pltpu.VMEM
    lanes = 128
    scratch = [v(hidden.shape, hidden.dtype)] + [v(w.shape, w.dtype) for w in big] + [
        v((model // lanes, lanes), BF16), v((1, rows), jnp.int32), v((1, rows), jnp.int32), v((1, lanes), F32),
        pltpu.SMEM((1, rows), jnp.int32),
        v((model // lanes, lanes), F32),
        v((rows, model), BF16),
        v((n, 8, lanes), F32),
        v((n, cap, t_width), BF16),
        v((n, cap, t_width), BF16),
        v((n * rows, s_width), BF16),
        v((n * rows, s_width), BF16),
        v((packs * cap, ranks2), F32),
        v((n_tp - 1, packs * cap, ranks2), F32),
        v((n * rows, total), BF16),
        v((n * rows, total), F32),
        v((n + 1, rows, total), BF16),
        v((rows, heads, HEAD_WIDTH), F32),
        v((rows, kv_heads, HEAD_WIDTH), F32),
        v((rows, kv_heads, HEAD_WIDTH), F32),
        v((rows, heads, HEAD_WIDTH), F32),
        v((n * rows, q_width), BF16),
        v((n * rows, s_width), BF16),
        v((n * rows, s_width), F32),
        v((chips, share, s_width), BF16),
        v((chips - 1, share, s_width), BF16),
        v((share, s_width), F32),
        v((chips - 1, share, s_width), BF16),
        dma, dma((5,)), dma((9,)),
        dma((n - 1,)), dma((n,)),
        dma((n - 1,)), dma((n,)),
        dma((n - 1,)), dma((n,)),
        dma((n,)), dma((n,)),
        dma((n_tp - 1,)), dma((n_tp - 1,)),
        dma((chunks, n - 1)), dma((chunks, n + 1)),
        dma((kv_heads * pieces, n)), dma((kv_heads * pieces, n)),
        dma((o_chunks, chips)), dma((o_chunks, chips)),
        dma((o_chunks, chips - 1)), dma((o_chunks, chips - 1)),
    ]
    shapes = [((share, s_width), BF16), ((rows, kv_width), BF16), ((rows, kv_width), BF16)]
    held = pl.pallas_call(
        functools.partial(kernel, n, n_tp),
        out_shape=[pltpu.VMEM(*one) for one in shapes],
        in_specs=[pl.BlockSpec(memory_space=pl.ANY)] * 14,
        out_specs=[vmem] * 3,
        scratch_shapes=scratch,
        compiler_params=pltpu.CompilerParams(
            collective_id=0, has_side_effects=True, vmem_limit_bytes=62 * 1024 * 1024
        ),
    )(
        hidden, input_norm_gain.reshape(model // lanes, lanes), request_adapter[None, :],
        cache_fill_length[None, :], frequency, *big,
    )
    return tuple(held)


def solution(mesh):
    return jax.shard_map(
        functools.partial(on_device, mesh.shape["ada"], mesh.shape["tp"]),
        mesh=mesh,
        in_specs=(
            P(("rep", "ada"), None),
            P(),
            P(("rep", "ada")),
            P(("rep", "ada")),
            P("ada", "tp"),
            P("ada", "tp"),
            P("ada", "tp"),
            P("tp", "ada"),
            P("tp", "ada"),
            P("ada", "tp"),
            P("ada", "tp"),
            P(("rep", "ada"), None, "tp"),
            P(("rep", "ada"), None, "tp"),
        ),
        out_specs=(P(("rep", "tp"), "ada"), P(("rep", "ada"), "tp"), P(("rep", "ada"), "tp")),
        check_vma=False,
    )
```

```python
import functools

import jax
import jax.numpy as jnp
import numpy as np
from jax import lax
from jax.experimental import pallas as pl
from jax.experimental.pallas import tpu as pltpu
from jax.sharding import PartitionSpec as P

QUERY_HEAD_COUNT = 64
KEY_VALUE_HEADS = 8
HEAD_WIDTH = 128
ADAPTER_RANK = 16
ADAPTER_SCALE = 2.0
EPSILON = 1e-05
ROPE_BASE = 500000.0
MESH = pl.DeviceIdType.MESH
F32 = jnp.float32
BF16 = jnp.bfloat16
GROUPS = QUERY_HEAD_COUNT // KEY_VALUE_HEADS
REQ_STEP = 16


def dot(a, b):
    return jnp.dot(a, b, preferred_element_type=F32)


def remote(src, dst, send, recv, target):
    return pltpu.make_async_remote_copy(
        src_ref=src, dst_ref=dst, send_sem=send, recv_sem=recv, device_id=target, device_id_type=MESH
    )


def kernel(
    n, n_tp,
    hid_h, gain_h, ids_h, fill_h, freq_h, qw_h, kw_h, vw_h, ow_h, dw_h, qu_h, vu_h, kc_h, vc_h,
    out, nk_out, nv_out,
    hid, qw, kvw, ow, dw, qu, vu, kvc,
    gain, ids_row, fill_row, freq, fill, wide_gain, normed, meta, route, rin, xin, xnorm, shr, shr_in, tsend, term, rs, rq3, nk3, nv3, ctx3, ctx,
    osend, oterm, opair, osum, oown, ors,
    small_sem, load_sem, send_sem, one_r, x_r, rs_r, ctx_r, out_r, far_r,
):
    a = lax.axis_index("ada")
    t = lax.axis_index("tp")
    core = lax.rem(t, 2)
    partner = t + 1 - 2 * core
    rows, model = hid.shape
    cap = route.shape[1]
    t_width, ranks2 = dw.shape
    s_width = xin.shape[1]
    half = s_width // 2
    q_width, kv_width = qw.shape[1], kvw.shape[2]
    kv_heads = kv_width // HEAD_WIDTH
    pieces, _, piece, _ = ctx.shape
    sub = oown.shape[1]
    meta_s, route_s, x_s, pair_s, shr_s, rs_s, ctx_s, out_s, far_s = [send_sem.at[i] for i in range(9)]
    meta_r, route_r, pair_r, shr_r = [one_r.at[i] for i in range(4)]
    chips = n_tp // 2
    chip = t // 2
    pair = 2 * ADAPTER_RANK
    held = ranks2 // pair
    step = 128
    relays = n > 3

    first = 1 - lax.div(a + n - 1, n)
    last = lax.div(a + 1, n)
    upper = lax.div(2 * a, n)
    is_end = jnp.logical_and(relays, jnp.logical_or(a == 0, a == n - 1))
    is_next = jnp.logical_and(relays, jnp.logical_or(a == 1, a == n - 2))
    end = (first + last) if relays else 0

    def peer(k):
        low = n - 1 - k
        low = low - lax.div(a - low + n, n)
        high = k + lax.div(k - a + n, n)
        return low + upper * (high - low)

    def block(index, size):
        return pl.ds(pl.multiple_of(index * size, size), size)

    def when(condition, action):
        if condition is True:
            action()
        elif condition is not False:
            pl.when(condition)(action)

    hid_load = pltpu.make_async_copy(hid_h, hid, load_sem.at[9])
    hid_load.start()
    small_loads = [
        pltpu.make_async_copy(src, dst, small_sem.at[i])
        for i, (src, dst) in enumerate(
            [(gain_h, gain), (ids_h, ids_row), (fill_h, fill_row), (freq_h, freq), (fill_h, fill)]
        )
    ]
    for load in small_loads:
        load.start()
    barrier = pltpu.get_barrier_semaphore()
    for d in range(1, n):
        pl.semaphore_signal(barrier, inc=1, device_id={"ada": lax.rem(a + d, n)}, device_id_type=MESH)
    for d in range(1, n_tp):
        pl.semaphore_signal(barrier, inc=1, device_id={"tp": lax.rem(t + d, n_tp)}, device_id_type=MESH)
    loads = [
        pltpu.make_async_copy(src, dst, load_sem.at[i])
        for i, (src, dst) in enumerate(
            [
                (dw_h, dw), (qu_h, qu), (vu_h, vu), (kw_h, kvw.at[0]), (vw_h, kvw.at[1]), (qw_h, qw),
                (kc_h, kvc.at[0]), (vc_h, kvc.at[1]), (ow_h, ow),
            ]
        )
    ]
    for load in loads:
        load.start()

    for load in small_loads:
        load.wait()
    wide_gain[...] = gain[...].astype(F32)
    diagonal = lax.broadcasted_iota(jnp.int32, (rows, 128), 0) == lax.broadcasted_iota(jnp.int32, (rows, 128), 1)
    square = diagonal[:, :rows]
    before = lax.broadcasted_iota(jnp.int32, (rows, rows), 0) < lax.broadcasted_iota(jnp.int32, (rows, rows), 1)

    def to_column(row):
        return jnp.sum(jnp.where(square, row, 0.0), axis=-1, keepdims=True)

    def to_row(column):
        return jnp.sum(jnp.where(diagonal, column, 0.0), axis=0, keepdims=True)

    row_id = ids_row[...].astype(F32)
    col_id = to_column(row_id)
    angles = to_column(fill_row[...].astype(F32)) * freq[...]
    cos_v, sin_v = jnp.cos(angles), jnp.sin(angles)
    sin_v = jnp.where(lax.broadcasted_iota(jnp.int32, sin_v.shape, 1) < HEAD_WIDTH // 2, -sin_v, sin_v)
    owner_row, owner_col = jnp.zeros_like(row_id), jnp.zeros_like(col_id)
    for o in range(1, n):
        owner_row = owner_row + (row_id >= o * held).astype(F32)
        owner_col = owner_col + (col_id >= o * held).astype(F32)
    slot_row = jnp.sum(jnp.where((owner_col == owner_row) & before, 1.0, 0.0), axis=0, keepdims=True)
    target = (owner_row * cap + slot_row).astype(jnp.int32)
    picker = jnp.where(
        lax.broadcasted_iota(jnp.int32, (n * cap, rows), 0) == target, 1.0, 0.0
    ).astype(BF16)
    if relays:
        @pl.when(is_end)
        def _():
            rs[peer(0)] = jnp.zeros(rs.shape[1:], rs.dtype)

    hid_load.wait()
    squares = jnp.zeros((rows, step), F32)
    for c in range(0, model, step):
        wide = hid[:, c : c + step].astype(F32)
        squares = squares + wide * wide
    inverse = lax.rsqrt(jnp.sum(squares, axis=-1, keepdims=True) / model + EPSILON)
    meta[a] = jnp.where(
        lax.broadcasted_iota(jnp.int32, (8, 128), 0) == 0, to_row(inverse), to_row(col_id)
    )
    for c in range(0, model, step):
        wide = hid[:, c : c + step].astype(F32)
        normed[:, c : c + step] = (wide * inverse * wide_gain[c // step : c // step + 1, :]).astype(BF16)
    route[...] = dot(picker, normed[:, block(t, t_width)]).astype(BF16).reshape(n, cap, t_width)
    rin[a] = route[a]
    my_rows = block(a, rows)
    my_half = block(core, half)
    xin[my_rows, :] = hid[:, block(a, s_width)]

    pl.semaphore_wait(barrier, n - 1 + n_tp - 1)
    for k in range(n - 1):
        to = peer(k)
        remote(meta.at[a], meta.at[a], meta_s, meta_r, {"ada": to}).start()
    for k in range(n - 1):
        to = peer(k)
        remote(route.at[to], rin.at[a], route_s, route_r, {"ada": to}).start()
    for k in reversed(range(n - 1)):
        to = peer(k)
        remote(
            hid.at[:, pl.ds(pl.multiple_of(to * s_width + core * half, 128), half)],
            xin.at[my_rows, my_half], x_s, x_r.at[a], {"ada": to},
        ).start()
    near_first = [peer(k) for k in reversed(range(n - 1))]

    def landed(dst, send, recv):
        remote(dst, dst, send, recv, {"ada": lax.rem(a + 1, n)}).wait_recv()

    def sent(src, send):
        remote(src, src, send, meta_r, {"ada": lax.rem(a + 1, n)}).wait_send()

    others = pl.ds(0, n - 1)
    other_rows = pl.ds(0, (n - 1) * rows)
    landed(meta.at[others], meta_s, meta_r)
    lane_cap = lax.broadcasted_iota(jnp.int32, (cap, ranks2), 1) // pair
    lane_rows = lax.broadcasted_iota(jnp.int32, (rows, ranks2), 1) // pair
    low_id = (a * held).astype(F32)
    places, slot_masks, id_cols, scales = [], [], [], []
    for s in range(n):
        ids_s = meta[s, 1:2, :rows]
        col_s = to_column(ids_s)
        here_row = (ids_s >= low_id) & (ids_s < low_id + held)
        here_col = (col_s >= low_id) & (col_s < low_id + held)
        slots = jnp.sum(jnp.where(here_col & before, 1.0, 0.0), axis=0, keepdims=True)
        chosen_slot = lax.broadcasted_iota(jnp.int32, (cap, rows), 0) == slots.astype(jnp.int32)
        slot_id = jnp.sum(jnp.where(chosen_slot & here_row, ids_s - low_id, 0.0), axis=-1, keepdims=True)
        slot_masks.append(lane_cap == slot_id.astype(jnp.int32))
        slot_col = to_column(slots).astype(jnp.int32)
        places.append(
            jnp.where((lax.broadcasted_iota(jnp.int32, (rows, cap), 1) == slot_col) & here_col, 1.0, 0.0).astype(BF16)
        )
        id_cols.append((col_s - low_id).astype(jnp.int32))
        scales.append(to_column(meta[s, 0:1, :rows]))
    row_ids = jnp.concatenate(id_cols, axis=0)

    loads[0].wait()
    landed(rin.at[others], route_s, route_r)
    partial = dot(rin[...].reshape(n * cap, t_width), dw[...])
    for first_s in range(0, n, held):
        tile = jnp.zeros((cap, ranks2), F32)
        for s in range(first_s, min(n, first_s + held)):
            picked = jnp.where(slot_masks[s], partial[s * cap : (s + 1) * cap], 0.0)
            folded = picked
            for i in range(1, held):
                folded = folded + pltpu.roll(picked, i * pair, 1)
            tile = jnp.where(lane_cap == s - first_s, folded, tile)
        shr[first_s // held * cap : (first_s // held + 1) * cap, :] = tile
    for d in range(1, n_tp):
        to = lax.rem(t + d, n_tp)
        remote(shr, shr_in.at[d - 1], shr_s, shr_r, {"tp": to}).start()

    def x_region(s):
        return xin.at[block(s, rows), my_half]

    for s in near_first:
        landed(x_region(s), x_s, x_r.at[s])
        remote(x_region(s), x_region(s), pair_s, pair_r, {"tp": partner}).start()

    landed(shr_in, shr_s, shr_r)
    total = shr[...]
    for d in range(1, n_tp):
        total = total + shr_in[d - 1]
    chosen = (total.astype(BF16).astype(F32) * ADAPTER_SCALE).astype(BF16)
    spread = []
    for s in range(n):
        mine = chosen[s // held * cap : (s // held + 1) * cap]
        spread.append(jnp.where(lane_rows == s % held, dot(places[s], mine), 0.0))
    spread = jnp.concatenate(spread, axis=0).astype(BF16)
    narrow = held * ADAPTER_RANK
    from_lane = lax.broadcasted_iota(jnp.int32, (ranks2, narrow), 0) % pair
    to_lane = lax.broadcasted_iota(jnp.int32, (ranks2, narrow), 1) % ADAPTER_RANK
    own_lane = lax.broadcasted_iota(jnp.int32, (n * rows, narrow), 1) // ADAPTER_RANK == row_ids
    ups = []
    for offset in (0, ADAPTER_RANK):
        moved = dot(spread, jnp.where(from_lane == to_lane + offset, 1.0, 0.0).astype(BF16))
        ups.append(jnp.where(own_lane, moved, 0.0).astype(BF16))

    landed(xin.at[other_rows, my_half], pair_s, pair_r)
    for s in range(n):
        rows_s = slice(s * rows, (s + 1) * rows)
        for c in range(0, s_width, step):
            gains = wide_gain[pl.ds(a * (s_width // step) + c // step, 1), :]
            xnorm[rows_s, c : c + step] = (xin[rows_s, c : c + step].astype(F32) * scales[s] * gains).astype(BF16)
    for load in loads[1:6]:
        load.wait()

    spare = n
    beside = first + last * (n - 2)
    far_target = peer(0) + end * (beside - peer(0))
    far_slot = a + end * (spare - a)
    chunks = []
    groups = 1 + kv_heads

    def of_group(index):
        return 0 if index == 0 else 1 + (index - 1) // per_g

    def chunk_copy(index, k):
        at, width = chunks[index]
        cols = pl.ds(at, width)
        to = peer(k)
        target, slot, mark_at = to, a, of_group(index)
        if k == 0:
            target, slot, mark_at = far_target, far_slot, mark_at + end * (groups + index - mark_at)
        return remote(
            tsend.at[block(to, rows), cols], rs.at[slot, :, cols], rs_s, rs_r.at[mark_at], {"ada": target}
        )

    def give(value, at, width):
        index = len(chunks)
        chunks.append((at, width))
        term[:, at : at + width] = value
        tsend[:, at : at + width] = value.astype(BF16)

    def ship(index, k):
        direct = k > 0 or not relays
        when(True if direct else jnp.logical_not(is_next), lambda: chunk_copy(index, k).start())

    def relay(index):
        if not relays:
            return
        at, width = chunks[index]
        cols = pl.ds(at, width)

        @pl.when(is_next)
        def _():
            landed(rs.at[spare, :, cols], rs_s, rs_r.at[groups + index])
            there = block(peer(0), rows)
            tsend[there, cols] = (term[there, cols] + rs[spare, :, cols].astype(F32)).astype(BF16)
            remote(
                tsend.at[there, cols], rs.at[a, :, cols], rs_s, rs_r.at[of_group(index)], {"ada": peer(0)}
            ).start()

    def arrived(group):
        cols = pl.ds(q_width, 2 * kv_width) if group == 0 else pl.ds((group - 1) * wide_g, wide_g)

        def take(count):
            landed(rs.at[pl.ds(0, count), :, cols], rs_s, rs_r.at[group])

        if not relays:
            take(n - 1)
        else:
            pl.when(is_end)(lambda: take(n - 2))
            pl.when(jnp.logical_not(is_end))(lambda: take(n - 1))

    wide_g = GROUPS * HEAD_WIDTH
    q_step = min(512, wide_g)
    per_g = wide_g // q_step
    x = xnorm[...]
    give(
        jnp.concatenate([dot(x, kvw[0]), dot(x, kvw[1]) + dot(ups[1], vu[...])], axis=1), q_width, 2 * kv_width
    )
    ship(0, 0)
    for g in range(kv_heads):
        group = range(1 + g * per_g, 1 + (g + 1) * per_g)
        for index in group:
            at = (index - 1) * q_step
            give(dot(x, qw[:, at : at + q_step]) + dot(ups[0], qu[:, at : at + q_step]), at, q_step)
            if g == 0:
                ship(index, 0)
        if g == 0:
            for k in range(1, n - 1):
                for index in [0, *group]:
                    ship(index, k)
    for index in range(1 + per_g):
        relay(index)
    for g in range(1, kv_heads):
        for k in range(n - 1):
            for index in range(1 + g * per_g, 1 + (g + 1) * per_g):
                ship(index, k)

    def summed(at, width):
        value = term[my_rows, at : at + width]
        for k in range(n - 1):
            value = value + rs[peer(k), :, at : at + width].astype(F32)
        return value

    def turn(value):
        return (value * cos_v + pltpu.roll(value, HEAD_WIDTH // 2, 1) * sin_v).astype(BF16)

    arrived(0)
    for h in range(kv_heads):
        cols = slice(h * HEAD_WIDTH, (h + 1) * HEAD_WIDTH)
        key = turn(summed(q_width + h * HEAD_WIDTH, HEAD_WIDTH))
        nk_out[:, cols] = key
        nk3[:, h, :] = key.astype(F32)
    for h in range(kv_heads):
        cols = slice(h * HEAD_WIDTH, (h + 1) * HEAD_WIDTH)
        fresh = summed(q_width + kv_width + h * HEAD_WIDTH, HEAD_WIDTH).astype(BF16)
        nv_out[:, cols] = fresh
        nv3[:, h, :] = fresh.astype(F32)
    score_scale = HEAD_WIDTH ** (-0.5)

    def attend(g, start):
        score_list, own_list, fill_list, val_list = [], [], [], []
        for j in range(REQ_STEP):
            r = start + j
            q = rq3[r, g * GROUPS : (g + 1) * GROUPS, :]
            keys = kvc[0, r, :, g * HEAD_WIDTH : (g + 1) * HEAD_WIDTH]
            score_list.append(
                lax.dot_general(q.astype(BF16), keys, (((1,), (1,)), ((), ())), preferred_element_type=F32)
            )
            own_list.append(jnp.sum(q * nk3[r, g : g + 1, :], axis=-1, keepdims=True))
            val_list.append(jnp.broadcast_to(nv3[r, g : g + 1, :], (GROUPS, HEAD_WIDTH)))
            fill_list.append(jnp.full((GROUPS, 1), fill[0, r], jnp.int32))
        scores = jnp.concatenate(score_list, axis=0) * score_scale
        own = jnp.concatenate(own_list, axis=0) * score_scale
        lengths = jnp.concatenate(fill_list, axis=0)
        inside = lax.broadcasted_iota(jnp.int32, scores.shape, 1) < lengths
        masked = jnp.where(inside, scores, -1e30)
        top = jnp.maximum(jnp.max(masked, axis=-1, keepdims=True), own)
        terms = jnp.where(inside, jnp.exp(masked - top), 0.0)
        own_exp = jnp.exp(own - top)
        scale = 1.0 / (jnp.sum(terms, axis=-1, keepdims=True) + own_exp)
        low = (terms * scale).astype(BF16)
        own_part = (own_exp * scale).astype(BF16).astype(F32) * jnp.concatenate(val_list, axis=0)
        for j in range(REQ_STEP):
            r = start + j
            values = kvc[1, r, :, g * HEAD_WIDTH : (g + 1) * HEAD_WIDTH]
            b = slice(j * GROUPS, (j + 1) * GROUPS)
            ctx3[r, g * GROUPS : (g + 1) * GROUPS, :] = dot(low[b], values) + own_part[b]

    def ctx_region(s, index):
        return ctx.at[index % pieces, s, :, pl.ds(index // pieces * wide_g, wide_g)]

    def ctx_send(index):
        here = ctx_region(a, index)
        for k in range(1 if relays else 0, n - 1):
            copy = remote(here, here, ctx_s, ctx_r.at[index, a], {"ada": peer(k)})
            when(jnp.logical_or(is_end, is_next) if relays and k == n - 2 else True, copy.start)

    def ctx_landed(index, k):
        landed(ctx_region(peer(k), index), ctx_s, ctx_r.at[index, peer(k)])

    def pass_on(index):
        if not relays:
            return

        @pl.when(is_next)
        def _():
            for k in reversed(range(n - 2)):
                there = ctx_region(peer(k), index)
                ctx_landed(index, k)
                remote(
                    there, there, ctx_s, ctx_r.at[index, peer(k)], {"ada": lax.div(a, n - 2) * (n - 1)}
                ).start()

    def gathered(index):
        for k in reversed(range(n - 1)):
            when(jnp.logical_not(is_next) if relays and k < n - 2 else True, lambda: ctx_landed(index, k))

    turned = 0
    for g in range(kv_heads):
        arrived(1 + g)
        while turned < (g + 1) * GROUPS:
            rq3[:, turned, :] = turn(summed(turned * HEAD_WIDTH, HEAD_WIDTH)).astype(F32)
            turned += 1
        if g < kv_heads - 1:
            for index in range(1 + (g + 1) * per_g, 1 + (g + 2) * per_g):
                relay(index)
        if g == 0:
            for load in loads[6:8]:
                load.wait()
        for p in range(pieces):
            @pl.loop(0, piece // REQ_STEP)
            def _(i):
                attend(g, p * piece + i * REQ_STEP)

            for h in range(g * GROUPS, (g + 1) * GROUPS):
                ctx[p, a, :, h * HEAD_WIDTH : (h + 1) * HEAD_WIDTH] = ctx3[
                    p * piece : (p + 1) * piece, h, :
                ].astype(BF16)
            index = g * pieces + p
            ctx_send(index)

    loads[8].wait()
    o_step = min(1024, s_width)
    o_chunks = s_width // o_step
    span = n * piece

    def to_partner(p, i):
        cols = pl.ds(i * o_step, o_step)
        for j in range(chips):
            mine = pl.ds(pl.multiple_of(p * span + (2 * j + 1 - core) * sub, sub), sub)
            remote(
                osend.at[mine, cols], opair.at[p, j, :, cols], out_s, out_r.at[p * o_chunks + i], {"tp": partner}
            ).start()

    def part_of(p, i, whose):
        at = slice(i * o_step, (i + 1) * o_step)
        there = pl.ds(pl.multiple_of(p * span + (2 * whose + core) * sub, sub), sub)
        return oterm[there, at] + opair[p, whose, :, at].astype(F32)

    def to_chips(p):
        for i in range(o_chunks):
            cols = pl.ds(i * o_step, o_step)
            landed(opair.at[p, :, :, cols], out_s, out_r.at[p * o_chunks + i])
            for e in range(1, chips):
                to = lax.rem(chip + e, chips)
                osum[p, e - 1, :, i * o_step : (i + 1) * o_step] = part_of(p, i, to).astype(BF16)
                remote(
                    osum.at[p, e - 1, :, cols], ors.at[p, e - 1, :, cols], far_s, far_r.at[p * o_chunks + i],
                    {"tp": 2 * to + core},
                ).start()

    for g in range(kv_heads - 1):
        for p in range(pieces):
            pass_on(g * pieces + p)
        for p in range(pieces):
            gathered(g * pieces + p)
        part = ctx[:, :, :, g * wide_g : (g + 1) * wide_g].reshape(pieces * span, wide_g)
        for at in range(0, s_width, o_step):
            value = dot(part, ow[g * wide_g : (g + 1) * wide_g, at : at + o_step])
            oterm[:, at : at + o_step] = value + oterm[:, at : at + o_step] if g > 0 else value
    g = kv_heads - 1
    for p in range(pieces):
        pass_on(g * pieces + p)
    for p in range(pieces):
        gathered(g * pieces + p)
        part = ctx[p, :, :, g * wide_g : (g + 1) * wide_g].reshape(span, wide_g)
        these = slice(p * span, (p + 1) * span)
        for i in range(o_chunks):
            at = i * o_step
            value = dot(part, ow[g * wide_g : (g + 1) * wide_g, at : at + o_step])
            if g > 0:
                value = value + oterm[these, at : at + o_step]
            oterm[these, at : at + o_step] = value
            osend[these, at : at + o_step] = value.astype(BF16)
            to_partner(p, i)
    for p in range(pieces):
        to_chips(p)

    homes = sub // piece
    for p in range(pieces):
        for i in range(o_chunks):
            cols = slice(i * o_step, (i + 1) * o_step)
            residual = jnp.concatenate(
                [
                    xin[pl.ds(pl.multiple_of((t * homes + h) * rows + p * piece, piece), piece), cols]
                    for h in range(homes)
                ],
                axis=0,
            )
            oown[p, :, cols] = residual.astype(F32) + part_of(p, i, chip)
    for p in range(pieces):
        for i in range(o_chunks):
            cols = slice(i * o_step, (i + 1) * o_step)
            landed(ors.at[p, :, :, pl.ds(i * o_step, o_step)], far_s, far_r.at[p * o_chunks + i])
            value = oown[p, :, cols]
            for e in range(1, chips):
                value = value + ors[p, e - 1, :, cols].astype(F32)
            for h in range(homes):
                out[h * rows + p * piece : h * rows + (p + 1) * piece, cols] = value[
                    h * piece : (h + 1) * piece
                ].astype(BF16)

    sent(meta.at[others], meta_s)
    sent(route.at[others], route_s)
    sent(xin.at[other_rows, my_half], x_s)
    sent(xin.at[other_rows, my_half], pair_s)
    sent(shr_in, shr_s)
    sent(tsend.at[other_rows], rs_s)
    if relays:
        sent(ctx.at[:, pl.ds(0, n - 3)], ctx_s)
        pl.when(jnp.logical_or(is_end, is_next))(lambda: sent(ctx.at[:, pl.ds(0, 1)], ctx_s))
        pl.when(is_next)(lambda: sent(ctx.at[:, pl.ds(0, n - 2)], ctx_s))
    else:
        sent(ctx.at[:, others], ctx_s)
    sent(osend.at[pl.ds(0, pieces * chips * sub)], out_s)
    sent(osum, far_s)


def put_out(*refs):
    sems = refs[6]
    copies = [pltpu.make_async_copy(refs[i], refs[3 + i], sems.at[i]) for i in range(3)]
    for copy in copies:
        copy.start()
    for copy in copies:
        copy.wait()


def on_device(
    n, n_tp, hidden, input_norm_gain, request_adapter, cache_fill_length, query_weight, key_weight,
    value_weight, output_weight, down_weight_all, query_up_weight, value_up_weight,
    rotated_key_cache, stored_value_cache,
):
    rows, model = hidden.shape
    q_width, kv_width = query_weight.shape[1], key_weight.shape[1]
    s_width, t_width = query_weight.shape[0], down_weight_all.shape[0]
    ranks2 = down_weight_all.shape[1]
    cap = max(2, (2 * rows + n - 1) // n)
    cap = (cap + 15) // 16 * 16
    share = n * rows // n_tp
    chips = n_tp // 2
    total = q_width + 2 * kv_width
    kv_heads, heads = kv_width // HEAD_WIDTH, q_width // HEAD_WIDTH
    halfway = HEAD_WIDTH // 2
    frequency = np.float32(ROPE_BASE) ** (np.float32(-2.0) * np.arange(halfway, dtype=np.float32) / np.float32(HEAD_WIDTH))
    frequency = jnp.asarray(np.concatenate([frequency, frequency])[None, :])
    big = [query_weight, key_weight, value_weight, output_weight, down_weight_all, query_up_weight,
           value_up_weight, rotated_key_cache, stored_value_cache]
    chunks = 1 + q_width // min(512, GROUPS * HEAD_WIDTH)
    o_chunks = s_width // min(1024, s_width)
    piece = min(16, rows)
    pieces = rows // piece
    per_pack = ranks2 // (2 * ADAPTER_RANK)
    packs = (n + per_pack - 1) // per_pack
    vmem = pl.BlockSpec(memory_space=pltpu.VMEM)
    dma = pltpu.SemaphoreType.DMA
    v = pltpu.VMEM
    lanes = 128
    scratch = [v(hidden.shape, hidden.dtype)] + [
        v(query_weight.shape, BF16), v((2, *key_weight.shape), BF16), v(output_weight.shape, BF16),
        v(down_weight_all.shape, BF16), v(query_up_weight.shape, BF16), v(value_up_weight.shape, BF16),
        v((2, *rotated_key_cache.shape), BF16),
        v((model // lanes, lanes), BF16), v((1, rows), jnp.int32), v((1, rows), jnp.int32), v((1, lanes), F32),
        pltpu.SMEM((1, rows), jnp.int32),
        v((model // lanes, lanes), F32),
        v((rows, model), BF16),
        v((n, 8, lanes), F32),
        v((n, cap, t_width), BF16),
        v((n, cap, t_width), BF16),
        v((n * rows, s_width), BF16),
        v((n * rows, s_width), BF16),
        v((packs * cap, ranks2), F32),
        v((n_tp - 1, packs * cap, ranks2), F32),
        v((n * rows, total), BF16),
        v((n * rows, total), F32),
        v((n + 1, rows, total), BF16),
        v((rows, heads, HEAD_WIDTH), F32),
        v((rows, kv_heads, HEAD_WIDTH), F32),
        v((rows, kv_heads, HEAD_WIDTH), F32),
        v((rows, heads, HEAD_WIDTH), F32),
        v((pieces, n, piece, q_width), BF16),
        v((n * rows, s_width), BF16),
        v((n * rows, s_width), F32),
        v((pieces, chips, share // pieces, s_width), BF16),
        v((pieces, chips - 1, share // pieces, s_width), BF16),
        v((pieces, share // pieces, s_width), F32),
        v((pieces, chips - 1, share // pieces, s_width), BF16),
        dma((5,)), dma((10,)), dma((9,)), dma((4,)), dma((n,)),
        dma((1 + kv_heads + chunks,)), dma((kv_heads * pieces, n)), dma((pieces * o_chunks,)),
        dma((pieces * o_chunks,)),
    ]
    shapes = [((share, s_width), BF16), ((rows, kv_width), BF16), ((rows, kv_width), BF16)]
    held = pl.pallas_call(
        functools.partial(kernel, n, n_tp),
        out_shape=[pltpu.VMEM(*one) for one in shapes],
        in_specs=[pl.BlockSpec(memory_space=pl.ANY)] * 14,
        out_specs=[vmem] * 3,
        scratch_shapes=scratch,
        compiler_params=pltpu.CompilerParams(
            collective_id=0, has_side_effects=True, vmem_limit_bytes=62 * 1024 * 1024
        ),
    )(
        hidden, input_norm_gain.reshape(model // lanes, lanes), request_adapter[None, :],
        cache_fill_length[None, :], frequency, *big,
    )
    held = [pltpu.with_memory_space_constraint(one, pltpu.VMEM) for one in held]
    return tuple(
        pl.pallas_call(
            put_out,
            out_shape=[jax.ShapeDtypeStruct(*one) for one in shapes],
            in_specs=[vmem] * 3,
            out_specs=[pl.BlockSpec(memory_space=pl.ANY)] * 3,
            scratch_shapes=[dma((3,))],
        )(*held)
    )


def solution(mesh):
    return jax.shard_map(
        functools.partial(on_device, mesh.shape["ada"], mesh.shape["tp"]),
        mesh=mesh,
        in_specs=(
            P(("rep", "ada"), None),
            P(),
            P(("rep", "ada")),
            P(("rep", "ada")),
            P("ada", "tp"),
            P("ada", "tp"),
            P("ada", "tp"),
            P("tp", "ada"),
            P("tp", "ada"),
            P("ada", "tp"),
            P("ada", "tp"),
            P(("rep", "ada"), None, "tp"),
            P(("rep", "ada"), None, "tp"),
        ),
        out_specs=(P(("rep", "tp"), "ada"), P(("rep", "ada"), "tp"), P(("rep", "ada"), "tp")),
        check_vma=False,
    )
```

```python
import functools

import jax
import jax.numpy as jnp
import numpy as np
from jax import lax
from jax.experimental import pallas as pl
from jax.experimental.pallas import tpu as pltpu
from jax.sharding import PartitionSpec as P

QUERY_HEAD_COUNT = 64
KEY_VALUE_HEADS = 8
HEAD_WIDTH = 128
ADAPTER_RANK = 16
ADAPTER_SCALE = 2.0
EPSILON = 1e-05
ROPE_BASE = 500000.0
MESH = pl.DeviceIdType.MESH
F32 = jnp.float32
BF16 = jnp.bfloat16
GROUPS = QUERY_HEAD_COUNT // KEY_VALUE_HEADS
REQ_STEP = 16


def dot(a, b):
    return jnp.dot(a, b, preferred_element_type=F32)


def remote(src, dst, send, recv, target):
    return pltpu.make_async_remote_copy(
        src_ref=src, dst_ref=dst, send_sem=send, recv_sem=recv, device_id=target, device_id_type=MESH
    )


def kernel(
    n, n_tp,
    hid_h, gain_h, ids_h, fill_h, freq_h, qw_h, kw_h, vw_h, ow_h, dw_h, qu_h, vu_h, kc_h, vc_h,
    out, nk_out, nv_out,
    hid, qw, kvw, ow, dw, qu, vu, kvc,
    gain, ids_row, fill_row, freq, fill, wide_gain, normed, meta, route, rin, xin, xnorm, shr, shr_in, tsend, term, rs, rq3, nk3, nv3, ctx3, ctx,
    osend, oterm, opair, osum, oown, ors,
    small_sem, load_sem, send_sem, one_r, x_r, rs_r, ctx_r, out_r, far_r,
):
    a = lax.axis_index("ada")
    t = lax.axis_index("tp")
    core = lax.rem(t, 2)
    partner = t + 1 - 2 * core
    rows, model = hid.shape
    cap = route.shape[1]
    t_width, ranks2 = dw.shape
    s_width = xin.shape[1]
    half = s_width // 2
    q_width, kv_width = qw.shape[1], kvw.shape[2]
    kv_heads = kv_width // HEAD_WIDTH
    pieces, _, piece, _ = ctx.shape
    sub = oown.shape[1]
    meta_s, route_s, x_s, pair_s, shr_s, rs_s, ctx_s, out_s, far_s = [send_sem.at[i] for i in range(9)]
    meta_r, route_r, pair_r, shr_r = [one_r.at[i] for i in range(4)]
    chips = n_tp // 2
    chip = t // 2
    pair = 2 * ADAPTER_RANK
    held = ranks2 // pair
    step = 128
    relays = n > 3

    first = 1 - lax.div(a + n - 1, n)
    last = lax.div(a + 1, n)
    upper = lax.div(2 * a, n)
    is_end = jnp.logical_and(relays, jnp.logical_or(a == 0, a == n - 1))
    is_next = jnp.logical_and(relays, jnp.logical_or(a == 1, a == n - 2))
    end = (first + last) if relays else 0

    def peer(k):
        low = n - 1 - k
        low = low - lax.div(a - low + n, n)
        high = k + lax.div(k - a + n, n)
        return low + upper * (high - low)

    def block(index, size):
        return pl.ds(pl.multiple_of(index * size, size), size)

    def when(condition, action):
        if condition is True:
            action()
        elif condition is not False:
            pl.when(condition)(action)

    hid_load = pltpu.make_async_copy(hid_h, hid, load_sem.at[9])
    hid_load.start()
    small_loads = [
        pltpu.make_async_copy(src, dst, small_sem.at[i])
        for i, (src, dst) in enumerate(
            [(gain_h, gain), (ids_h, ids_row), (fill_h, fill_row), (freq_h, freq), (fill_h, fill)]
        )
    ]
    for load in small_loads:
        load.start()
    barrier = pltpu.get_barrier_semaphore()
    for d in range(1, n):
        pl.semaphore_signal(barrier, inc=1, device_id={"ada": lax.rem(a + d, n)}, device_id_type=MESH)
    for d in range(1, n_tp):
        pl.semaphore_signal(barrier, inc=1, device_id={"tp": lax.rem(t + d, n_tp)}, device_id_type=MESH)
    loads = [
        pltpu.make_async_copy(src, dst, load_sem.at[i])
        for i, (src, dst) in enumerate(
            [
                (dw_h, dw), (qu_h, qu), (vu_h, vu), (kw_h, kvw.at[0]), (vw_h, kvw.at[1]), (qw_h, qw),
                (kc_h, kvc.at[0]), (vc_h, kvc.at[1]), (ow_h, ow),
            ]
        )
    ]
    for load in loads:
        load.start()

    for load in small_loads:
        load.wait()
    wide_gain[...] = gain[...].astype(F32)
    diagonal = lax.broadcasted_iota(jnp.int32, (rows, 128), 0) == lax.broadcasted_iota(jnp.int32, (rows, 128), 1)
    square = diagonal[:, :rows]
    before = lax.broadcasted_iota(jnp.int32, (rows, rows), 0) < lax.broadcasted_iota(jnp.int32, (rows, rows), 1)

    def to_column(row):
        return jnp.sum(jnp.where(square, row, 0.0), axis=-1, keepdims=True)

    def to_row(column):
        return jnp.sum(jnp.where(diagonal, column, 0.0), axis=0, keepdims=True)

    row_id = ids_row[...].astype(F32)
    col_id = to_column(row_id)
    angles = to_column(fill_row[...].astype(F32)) * freq[...]
    cos_v, sin_v = jnp.cos(angles), jnp.sin(angles)
    sin_v = jnp.where(lax.broadcasted_iota(jnp.int32, sin_v.shape, 1) < HEAD_WIDTH // 2, -sin_v, sin_v)
    owner_row, owner_col = jnp.zeros_like(row_id), jnp.zeros_like(col_id)
    for o in range(1, n):
        owner_row = owner_row + (row_id >= o * held).astype(F32)
        owner_col = owner_col + (col_id >= o * held).astype(F32)
    slot_row = jnp.sum(jnp.where((owner_col == owner_row) & before, 1.0, 0.0), axis=0, keepdims=True)
    target = (owner_row * cap + slot_row).astype(jnp.int32)
    picker = jnp.where(
        lax.broadcasted_iota(jnp.int32, (n * cap, rows), 0) == target, 1.0, 0.0
    ).astype(BF16)
    if relays:
        @pl.when(is_end)
        def _():
            rs[peer(0)] = jnp.zeros(rs.shape[1:], rs.dtype)

    hid_load.wait()
    squares = jnp.zeros((rows, step), F32)
    for c in range(0, model, step):
        wide = hid[:, c : c + step].astype(F32)
        squares = squares + wide * wide
    inverse = lax.rsqrt(jnp.sum(squares, axis=-1, keepdims=True) / model + EPSILON)
    meta[a] = jnp.where(
        lax.broadcasted_iota(jnp.int32, (8, 128), 0) == 0, to_row(inverse), to_row(col_id)
    )
    for c in range(0, model, step):
        wide = hid[:, c : c + step].astype(F32)
        normed[:, c : c + step] = (wide * inverse * wide_gain[c // step : c // step + 1, :]).astype(BF16)
    route[...] = dot(picker, normed[:, block(t, t_width)]).astype(BF16).reshape(n, cap, t_width)
    rin[a] = route[a]
    my_rows = block(a, rows)
    my_half = block(core, half)
    xin[my_rows, :] = hid[:, block(a, s_width)]

    pl.semaphore_wait(barrier, n - 1 + n_tp - 1)
    for k in range(n - 1):
        to = peer(k)
        remote(meta.at[a], meta.at[a], meta_s, meta_r, {"ada": to}).start()

    def send_route(k):
        to = peer(k)
        remote(route.at[to], rin.at[a], route_s, route_r, {"ada": to}).start()

    def send_x(k):
        to = peer(k)
        remote(
            hid.at[:, pl.ds(pl.multiple_of(to * s_width + core * half, 128), half)],
            xin.at[my_rows, my_half], x_s, x_r.at[a], {"ada": to},
        ).start()

    near_first = [peer(k) for k in reversed(range(n - 1))]

    def landed(dst, send, recv):
        remote(dst, dst, send, recv, {"ada": lax.rem(a + 1, n)}).wait_recv()

    def sent(src, send):
        remote(src, src, send, meta_r, {"ada": lax.rem(a + 1, n)}).wait_send()

    others = pl.ds(0, n - 1)
    other_rows = pl.ds(0, (n - 1) * rows)
    def outer():
        send_route(n - 2)
        send_x(n - 2)
        for k in range(n - 2):
            send_route(k)
        for k in reversed(range(n - 2)):
            send_x(k)

    def beside_end():
        send_route(n - 2)
        for k in range(n - 2):
            send_route(k)
        sent(route.at[others], route_s)
        send_x(n - 2)
        for k in reversed(range(n - 2)):
            send_x(k)

    if relays:
        pl.when(is_next)(beside_end)
        pl.when(jnp.logical_not(is_next))(outer)
    else:
        outer()
    landed(meta.at[others], meta_s, meta_r)
    lane_cap = lax.broadcasted_iota(jnp.int32, (cap, ranks2), 1) // pair
    lane_rows = lax.broadcasted_iota(jnp.int32, (rows, ranks2), 1) // pair
    low_id = (a * held).astype(F32)
    places, slot_masks, id_cols, scales = [], [], [], []
    for s in range(n):
        ids_s = meta[s, 1:2, :rows]
        col_s = to_column(ids_s)
        here_row = (ids_s >= low_id) & (ids_s < low_id + held)
        here_col = (col_s >= low_id) & (col_s < low_id + held)
        slots = jnp.sum(jnp.where(here_col & before, 1.0, 0.0), axis=0, keepdims=True)
        chosen_slot = lax.broadcasted_iota(jnp.int32, (cap, rows), 0) == slots.astype(jnp.int32)
        slot_id = jnp.sum(jnp.where(chosen_slot & here_row, ids_s - low_id, 0.0), axis=-1, keepdims=True)
        slot_masks.append(lane_cap == slot_id.astype(jnp.int32))
        slot_col = to_column(slots).astype(jnp.int32)
        places.append(
            jnp.where((lax.broadcasted_iota(jnp.int32, (rows, cap), 1) == slot_col) & here_col, 1.0, 0.0).astype(BF16)
        )
        id_cols.append((col_s - low_id).astype(jnp.int32))
        scales.append(to_column(meta[s, 0:1, :rows]))
    row_ids = jnp.concatenate(id_cols, axis=0)

    loads[0].wait()
    landed(rin.at[others], route_s, route_r)
    partial = dot(rin[...].reshape(n * cap, t_width), dw[...])
    for first_s in range(0, n, held):
        tile = jnp.zeros((cap, ranks2), F32)
        for s in range(first_s, min(n, first_s + held)):
            picked = jnp.where(slot_masks[s], partial[s * cap : (s + 1) * cap], 0.0)
            folded = picked
            for i in range(1, held):
                folded = folded + pltpu.roll(picked, i * pair, 1)
            tile = jnp.where(lane_cap == s - first_s, folded, tile)
        shr[first_s // held * cap : (first_s // held + 1) * cap, :] = tile
    for d in range(1, n_tp):
        to = lax.rem(t + d, n_tp)
        remote(shr, shr_in.at[d - 1], shr_s, shr_r, {"tp": to}).start()

    def x_region(s):
        return xin.at[block(s, rows), my_half]

    for s in near_first:
        landed(x_region(s), x_s, x_r.at[s])
        remote(x_region(s), x_region(s), pair_s, pair_r, {"tp": partner}).start()

    landed(shr_in, shr_s, shr_r)
    total = shr[...]
    for d in range(1, n_tp):
        total = total + shr_in[d - 1]
    chosen = (total.astype(BF16).astype(F32) * ADAPTER_SCALE).astype(BF16)
    spread = []
    for s in range(n):
        mine = chosen[s // held * cap : (s // held + 1) * cap]
        spread.append(jnp.where(lane_rows == s % held, dot(places[s], mine), 0.0))
    spread = jnp.concatenate(spread, axis=0).astype(BF16)
    narrow = held * ADAPTER_RANK
    from_lane = lax.broadcasted_iota(jnp.int32, (ranks2, narrow), 0) % pair
    to_lane = lax.broadcasted_iota(jnp.int32, (ranks2, narrow), 1) % ADAPTER_RANK
    own_lane = lax.broadcasted_iota(jnp.int32, (n * rows, narrow), 1) // ADAPTER_RANK == row_ids
    ups = []
    for offset in (0, ADAPTER_RANK):
        moved = dot(spread, jnp.where(from_lane == to_lane + offset, 1.0, 0.0).astype(BF16))
        ups.append(jnp.where(own_lane, moved, 0.0).astype(BF16))

    landed(xin.at[other_rows, my_half], pair_s, pair_r)
    for s in range(n):
        rows_s = slice(s * rows, (s + 1) * rows)
        for c in range(0, s_width, step):
            gains = wide_gain[pl.ds(a * (s_width // step) + c // step, 1), :]
            xnorm[rows_s, c : c + step] = (xin[rows_s, c : c + step].astype(F32) * scales[s] * gains).astype(BF16)
    for load in loads[1:6]:
        load.wait()

    spare = n
    beside = first + last * (n - 2)
    far_target = peer(0) + end * (beside - peer(0))
    far_slot = a + end * (spare - a)
    chunks = []
    groups = 1 + kv_heads

    def of_group(index):
        return 0 if index == 0 else 1 + (index - 1) // per_g

    def chunk_copy(index, k):
        at, width = chunks[index]
        cols = pl.ds(at, width)
        to = peer(k)
        target, slot, mark_at = to, a, of_group(index)
        if k == 0:
            target, slot, mark_at = far_target, far_slot, mark_at + end * (groups + index - mark_at)
        return remote(
            tsend.at[block(to, rows), cols], rs.at[slot, :, cols], rs_s, rs_r.at[mark_at], {"ada": target}
        )

    def give(value, at, width):
        index = len(chunks)
        chunks.append((at, width))
        term[:, at : at + width] = value
        tsend[:, at : at + width] = value.astype(BF16)

    def ship(index, k):
        direct = k > 0 or not relays
        when(True if direct else jnp.logical_not(is_next), lambda: chunk_copy(index, k).start())

    def relay(index):
        if not relays:
            return
        at, width = chunks[index]
        cols = pl.ds(at, width)

        @pl.when(is_next)
        def _():
            landed(rs.at[spare, :, cols], rs_s, rs_r.at[groups + index])
            there = block(peer(0), rows)
            tsend[there, cols] = (term[there, cols] + rs[spare, :, cols].astype(F32)).astype(BF16)
            remote(
                tsend.at[there, cols], rs.at[a, :, cols], rs_s, rs_r.at[of_group(index)], {"ada": peer(0)}
            ).start()

    def arrived(group):
        cols = pl.ds(q_width, 2 * kv_width) if group == 0 else pl.ds((group - 1) * wide_g, wide_g)

        def take(count):
            landed(rs.at[pl.ds(0, count), :, cols], rs_s, rs_r.at[group])

        if not relays:
            take(n - 1)
        else:
            pl.when(is_end)(lambda: take(n - 2))
            pl.when(jnp.logical_not(is_end))(lambda: take(n - 1))

    wide_g = GROUPS * HEAD_WIDTH
    q_step = min(512, wide_g)
    per_g = wide_g // q_step
    x = xnorm[...]
    give(
        jnp.concatenate([dot(x, kvw[0]), dot(x, kvw[1]) + dot(ups[1], vu[...])], axis=1), q_width, 2 * kv_width
    )
    ship(0, 0)
    for g in range(kv_heads):
        group = range(1 + g * per_g, 1 + (g + 1) * per_g)
        for index in group:
            at = (index - 1) * q_step
            give(dot(x, qw[:, at : at + q_step]) + dot(ups[0], qu[:, at : at + q_step]), at, q_step)
            if g == 0:
                ship(index, 0)
        if g == 0:
            for k in range(1, n - 1):
                for index in [0, *group]:
                    ship(index, k)
    for index in range(1 + per_g):
        relay(index)
    for g in range(1, kv_heads):
        for k in range(n - 1):
            for index in range(1 + g * per_g, 1 + (g + 1) * per_g):
                ship(index, k)

    def summed(at, width):
        value = term[my_rows, at : at + width]
        for k in range(n - 1):
            value = value + rs[peer(k), :, at : at + width].astype(F32)
        return value

    def turn(value):
        return (value * cos_v + pltpu.roll(value, HEAD_WIDTH // 2, 1) * sin_v).astype(BF16)

    arrived(0)
    for h in range(kv_heads):
        cols = slice(h * HEAD_WIDTH, (h + 1) * HEAD_WIDTH)
        key = turn(summed(q_width + h * HEAD_WIDTH, HEAD_WIDTH))
        nk_out[:, cols] = key
        nk3[:, h, :] = key.astype(F32)
    for h in range(kv_heads):
        cols = slice(h * HEAD_WIDTH, (h + 1) * HEAD_WIDTH)
        fresh = summed(q_width + kv_width + h * HEAD_WIDTH, HEAD_WIDTH).astype(BF16)
        nv_out[:, cols] = fresh
        nv3[:, h, :] = fresh.astype(F32)
    score_scale = HEAD_WIDTH ** (-0.5)

    def attend(g, start):
        score_list, own_list, fill_list, val_list = [], [], [], []
        for j in range(REQ_STEP):
            r = start + j
            q = rq3[r, g * GROUPS : (g + 1) * GROUPS, :]
            keys = kvc[0, r, :, g * HEAD_WIDTH : (g + 1) * HEAD_WIDTH]
            score_list.append(
                lax.dot_general(q.astype(BF16), keys, (((1,), (1,)), ((), ())), preferred_element_type=F32)
            )
            own_list.append(jnp.sum(q * nk3[r, g : g + 1, :], axis=-1, keepdims=True))
            val_list.append(jnp.broadcast_to(nv3[r, g : g + 1, :], (GROUPS, HEAD_WIDTH)))
            fill_list.append(jnp.full((GROUPS, 1), fill[0, r], jnp.int32))
        scores = jnp.concatenate(score_list, axis=0) * score_scale
        own = jnp.concatenate(own_list, axis=0) * score_scale
        lengths = jnp.concatenate(fill_list, axis=0)
        inside = lax.broadcasted_iota(jnp.int32, scores.shape, 1) < lengths
        masked = jnp.where(inside, scores, -1e30)
        top = jnp.maximum(jnp.max(masked, axis=-1, keepdims=True), own)
        terms = jnp.where(inside, jnp.exp(masked - top), 0.0)
        own_exp = jnp.exp(own - top)
        scale = 1.0 / (jnp.sum(terms, axis=-1, keepdims=True) + own_exp)
        low = (terms * scale).astype(BF16)
        own_part = (own_exp * scale).astype(BF16).astype(F32) * jnp.concatenate(val_list, axis=0)
        for j in range(REQ_STEP):
            r = start + j
            values = kvc[1, r, :, g * HEAD_WIDTH : (g + 1) * HEAD_WIDTH]
            b = slice(j * GROUPS, (j + 1) * GROUPS)
            ctx3[r, g * GROUPS : (g + 1) * GROUPS, :] = dot(low[b], values) + own_part[b]

    def ctx_region(s, index):
        return ctx.at[index % pieces, s, :, pl.ds(index // pieces * wide_g, wide_g)]

    def ctx_send(index):
        here = ctx_region(a, index)
        for k in range(n - 1):
            copy = remote(here, here, ctx_s, ctx_r.at[index, a], {"ada": peer(k)})
            when(jnp.logical_not(is_end) if relays and k == 0 else True, copy.start)

    def ctx_landed(index, k):
        landed(ctx_region(peer(k), index), ctx_s, ctx_r.at[index, peer(k)])

    def pass_on(index):
        if not relays:
            return

        @pl.when(is_next)
        def _():
            there = ctx_region(peer(0), index)
            ctx_landed(index, 0)
            remote(
                there, there, ctx_s, ctx_r.at[index, peer(0)], {"ada": lax.div(a, n - 2) * (n - 1)}
            ).start()

    def gathered(index):
        for k in reversed(range(n - 1)):
            when(jnp.logical_not(is_next) if relays and k == 0 else True, lambda: ctx_landed(index, k))

    turned = 0
    for g in range(kv_heads):
        arrived(1 + g)
        while turned < (g + 1) * GROUPS:
            rq3[:, turned, :] = turn(summed(turned * HEAD_WIDTH, HEAD_WIDTH)).astype(F32)
            turned += 1
        if g < kv_heads - 1:
            for index in range(1 + (g + 1) * per_g, 1 + (g + 2) * per_g):
                relay(index)
        if g == 0:
            for load in loads[6:8]:
                load.wait()
        for p in range(pieces):
            @pl.loop(0, piece // REQ_STEP)
            def _(i):
                attend(g, p * piece + i * REQ_STEP)

            for h in range(g * GROUPS, (g + 1) * GROUPS):
                ctx[p, a, :, h * HEAD_WIDTH : (h + 1) * HEAD_WIDTH] = ctx3[
                    p * piece : (p + 1) * piece, h, :
                ].astype(BF16)
            index = g * pieces + p
            ctx_send(index)

    loads[8].wait()
    o_step = min(1024, s_width)
    o_chunks = s_width // o_step
    span = n * piece

    def to_partner(p, i):
        cols = pl.ds(i * o_step, o_step)
        for j in range(chips):
            mine = pl.ds(pl.multiple_of(p * span + (2 * j + 1 - core) * sub, sub), sub)
            remote(
                osend.at[mine, cols], opair.at[p, j, :, cols], out_s, out_r.at[p * o_chunks + i], {"tp": partner}
            ).start()

    def part_of(p, i, whose):
        at = slice(i * o_step, (i + 1) * o_step)
        there = pl.ds(pl.multiple_of(p * span + (2 * whose + core) * sub, sub), sub)
        return oterm[there, at] + opair[p, whose, :, at].astype(F32)

    def to_chips(p):
        for i in range(o_chunks):
            cols = pl.ds(i * o_step, o_step)
            landed(opair.at[p, :, :, cols], out_s, out_r.at[p * o_chunks + i])
            for e in range(1, chips):
                to = lax.rem(chip + e, chips)
                osum[p, e - 1, :, i * o_step : (i + 1) * o_step] = part_of(p, i, to).astype(BF16)
                remote(
                    osum.at[p, e - 1, :, cols], ors.at[p, e - 1, :, cols], far_s, far_r.at[p * o_chunks + i],
                    {"tp": 2 * to + core},
                ).start()

    for g in range(kv_heads - 1):
        for p in range(pieces):
            pass_on(g * pieces + p)
        for p in range(pieces):
            gathered(g * pieces + p)
        part = ctx[:, :, :, g * wide_g : (g + 1) * wide_g].reshape(pieces * span, wide_g)
        for at in range(0, s_width, o_step):
            value = dot(part, ow[g * wide_g : (g + 1) * wide_g, at : at + o_step])
            oterm[:, at : at + o_step] = value + oterm[:, at : at + o_step] if g > 0 else value
    g = kv_heads - 1
    for p in range(pieces):
        pass_on(g * pieces + p)
    for p in range(pieces):
        gathered(g * pieces + p)
        part = ctx[p, :, :, g * wide_g : (g + 1) * wide_g].reshape(span, wide_g)
        these = slice(p * span, (p + 1) * span)
        for i in range(o_chunks):
            at = i * o_step
            value = dot(part, ow[g * wide_g : (g + 1) * wide_g, at : at + o_step])
            if g > 0:
                value = value + oterm[these, at : at + o_step]
            oterm[these, at : at + o_step] = value
            osend[these, at : at + o_step] = value.astype(BF16)
            to_partner(p, i)
            if p > 0 and i == 0:
                pl.when(core == 0)(lambda: to_chips(p - 1))
        if p > 0:
            pl.when(core == 1)(lambda: to_chips(p - 1))
    to_chips(pieces - 1)

    homes = sub // piece
    for p in range(pieces):
        for i in range(o_chunks):
            cols = slice(i * o_step, (i + 1) * o_step)
            residual = jnp.concatenate(
                [
                    xin[pl.ds(pl.multiple_of((t * homes + h) * rows + p * piece, piece), piece), cols]
                    for h in range(homes)
                ],
                axis=0,
            )
            oown[p, :, cols] = residual.astype(F32) + part_of(p, i, chip)
    for p in range(pieces):
        for i in range(o_chunks):
            cols = slice(i * o_step, (i + 1) * o_step)
            landed(ors.at[p, :, :, pl.ds(i * o_step, o_step)], far_s, far_r.at[p * o_chunks + i])
            value = oown[p, :, cols]
            for e in range(1, chips):
                value = value + ors[p, e - 1, :, cols].astype(F32)
            for h in range(homes):
                out[h * rows + p * piece : h * rows + (p + 1) * piece, cols] = value[
                    h * piece : (h + 1) * piece
                ].astype(BF16)

    sent(meta.at[others], meta_s)
    when(jnp.logical_not(is_next) if relays else True, lambda: sent(route.at[others], route_s))
    sent(xin.at[other_rows, my_half], x_s)
    sent(xin.at[other_rows, my_half], pair_s)
    sent(shr_in, shr_s)
    sent(tsend.at[other_rows], rs_s)
    if relays:
        pl.when(is_end)(lambda: sent(ctx.at[:, pl.ds(0, n - 2)], ctx_s))
        pl.when(is_next)(lambda: sent(ctx, ctx_s))
        inner = jnp.logical_not(jnp.logical_or(is_end, is_next))
        pl.when(inner)(lambda: sent(ctx.at[:, others], ctx_s))
    else:
        sent(ctx.at[:, others], ctx_s)
    sent(osend.at[pl.ds(0, pieces * chips * sub)], out_s)
    sent(osum, far_s)


def put_out(*refs):
    sems = refs[6]
    copies = [pltpu.make_async_copy(refs[i], refs[3 + i], sems.at[i]) for i in range(3)]
    for copy in copies:
        copy.start()
    for copy in copies:
        copy.wait()


def on_device(
    n, n_tp, hidden, input_norm_gain, request_adapter, cache_fill_length, query_weight, key_weight,
    value_weight, output_weight, down_weight_all, query_up_weight, value_up_weight,
    rotated_key_cache, stored_value_cache,
):
    rows, model = hidden.shape
    q_width, kv_width = query_weight.shape[1], key_weight.shape[1]
    s_width, t_width = query_weight.shape[0], down_weight_all.shape[0]
    ranks2 = down_weight_all.shape[1]
    cap = max(2, (2 * rows + n - 1) // n)
    cap = (cap + 15) // 16 * 16
    share = n * rows // n_tp
    chips = n_tp // 2
    total = q_width + 2 * kv_width
    kv_heads, heads = kv_width // HEAD_WIDTH, q_width // HEAD_WIDTH
    halfway = HEAD_WIDTH // 2
    frequency = np.float32(ROPE_BASE) ** (np.float32(-2.0) * np.arange(halfway, dtype=np.float32) / np.float32(HEAD_WIDTH))
    frequency = jnp.asarray(np.concatenate([frequency, frequency])[None, :])
    big = [query_weight, key_weight, value_weight, output_weight, down_weight_all, query_up_weight,
           value_up_weight, rotated_key_cache, stored_value_cache]
    chunks = 1 + q_width // min(512, GROUPS * HEAD_WIDTH)
    o_chunks = s_width // min(1024, s_width)
    piece = min(16, rows)
    pieces = rows // piece
    per_pack = ranks2 // (2 * ADAPTER_RANK)
    packs = (n + per_pack - 1) // per_pack
    vmem = pl.BlockSpec(memory_space=pltpu.VMEM)
    dma = pltpu.SemaphoreType.DMA
    v = pltpu.VMEM
    lanes = 128
    scratch = [v(hidden.shape, hidden.dtype)] + [
        v(query_weight.shape, BF16), v((2, *key_weight.shape), BF16), v(output_weight.shape, BF16),
        v(down_weight_all.shape, BF16), v(query_up_weight.shape, BF16), v(value_up_weight.shape, BF16),
        v((2, *rotated_key_cache.shape), BF16),
        v((model // lanes, lanes), BF16), v((1, rows), jnp.int32), v((1, rows), jnp.int32), v((1, lanes), F32),
        pltpu.SMEM((1, rows), jnp.int32),
        v((model // lanes, lanes), F32),
        v((rows, model), BF16),
        v((n, 8, lanes), F32),
        v((n, cap, t_width), BF16),
        v((n, cap, t_width), BF16),
        v((n * rows, s_width), BF16),
        v((n * rows, s_width), BF16),
        v((packs * cap, ranks2), F32),
        v((n_tp - 1, packs * cap, ranks2), F32),
        v((n * rows, total), BF16),
        v((n * rows, total), F32),
        v((n + 1, rows, total), BF16),
        v((rows, heads, HEAD_WIDTH), F32),
        v((rows, kv_heads, HEAD_WIDTH), F32),
        v((rows, kv_heads, HEAD_WIDTH), F32),
        v((rows, heads, HEAD_WIDTH), F32),
        v((pieces, n, piece, q_width), BF16),
        v((n * rows, s_width), BF16),
        v((n * rows, s_width), F32),
        v((pieces, chips, share // pieces, s_width), BF16),
        v((pieces, chips - 1, share // pieces, s_width), BF16),
        v((pieces, share // pieces, s_width), F32),
        v((pieces, chips - 1, share // pieces, s_width), BF16),
        dma((5,)), dma((10,)), dma((9,)), dma((4,)), dma((n,)),
        dma((1 + kv_heads + chunks,)), dma((kv_heads * pieces, n)), dma((pieces * o_chunks,)),
        dma((pieces * o_chunks,)),
    ]
    shapes = [((share, s_width), BF16), ((rows, kv_width), BF16), ((rows, kv_width), BF16)]
    held = pl.pallas_call(
        functools.partial(kernel, n, n_tp),
        out_shape=[pltpu.VMEM(*one) for one in shapes],
        in_specs=[pl.BlockSpec(memory_space=pl.ANY)] * 14,
        out_specs=[vmem] * 3,
        scratch_shapes=scratch,
        compiler_params=pltpu.CompilerParams(
            collective_id=0, has_side_effects=True, vmem_limit_bytes=62 * 1024 * 1024
        ),
    )(
        hidden, input_norm_gain.reshape(model // lanes, lanes), request_adapter[None, :],
        cache_fill_length[None, :], frequency, *big,
    )
    held = [pltpu.with_memory_space_constraint(one, pltpu.VMEM) for one in held]
    return tuple(
        pl.pallas_call(
            put_out,
            out_shape=[jax.ShapeDtypeStruct(*one) for one in shapes],
            in_specs=[vmem] * 3,
            out_specs=[pl.BlockSpec(memory_space=pl.ANY)] * 3,
            scratch_shapes=[dma((3,))],
        )(*held)
    )


def solution(mesh):
    return jax.shard_map(
        functools.partial(on_device, mesh.shape["ada"], mesh.shape["tp"]),
        mesh=mesh,
        in_specs=(
            P(("rep", "ada"), None),
            P(),
            P(("rep", "ada")),
            P(("rep", "ada")),
            P("ada", "tp"),
            P("ada", "tp"),
            P("ada", "tp"),
            P("tp", "ada"),
            P("tp", "ada"),
            P("ada", "tp"),
            P("ada", "tp"),
            P(("rep", "ada"), None, "tp"),
            P(("rep", "ada"), None, "tp"),
        ),
        out_specs=(P(("rep", "tp"), "ada"), P(("rep", "ada"), "tp"), P(("rep", "ada"), "tp")),
        check_vma=False,
    )
```
